32 devices in a mesh: dp: 8 (over y, x, core), seq: 4 (over z).
Axes of the slice: x: 2, y: 2, z: 4, core: 2. Of those that a mesh axis runs over, the one named last changes fastest.
Arguments:
- tokens: bfloat16 [8, 512, 1024], P('dp', 'seq'), may hold values from -6 to 6
- cotangent: bfloat16 [8, 512, 1024], P('dp', 'seq'), may hold values from -6 to 6
- stamps: int32 [8, 512], P('dp'), may hold values from 0 to 1080832, as said below
- lengths: int32 [8], P('dp'), may hold values from 64 to 512, as said below
- w_qkvu: bfloat16 [1024, 4096], P('dp'), may hold values from -0.1875 to 0.1875
- w_out: bfloat16 [1024, 1024], P('dp'), may hold values from -0.1875 to 0.1875
- gain_in: float32 [1024], replicated, may hold values from 0.25 to 1.75
- gain_out: float32 [1024], replicated, may hold values from 0.25 to 1.75
- bias_table: float32 [8, 16], replicated, may hold values from -4 to 4
Outputs:
- mixed: bfloat16 [8, 512, 1024], P('dp', 'seq')
- input_grad: bfloat16 [8, 512, 1024], P('dp', 'seq')
- out_weight_grad: float32 [1024, 1024], P('dp')
The draws below stay inside these ranges and needn't reach their ends.
Inputs may be any that keep to these rules, and one draw needn't show every extreme that they name: `lengths`: each stream has 64 valid actions or more; some stream is full. `stamps`: timestamps never fall along a stream, and consecutive ones differ by less than 64.
All inputs are finite; a program needn't handle non-finite values.
Results may differ from the reference program's by a relative error of at most 0.019.
Values may be sent and summed in bfloat16 or wider, within the bound.
A program may use at most 128 MiB of HBM per device.

```python
import jax
import jax.numpy as jnp
from jax import lax

D = 1024
H = 8
DH = 128
NB = 16
TOK_DEV = 128
SEQLEN = 512
STREAMS = 8
N_SEQ = 4


def draw_lengths(key, part):
    spread = jax.random.randint(key, (STREAMS,), SEQLEN // 8, SEQLEN + 1)
    chosen = jax.random.randint(jax.random.fold_in(key, 7), (), 0, STREAMS)
    return jnp.where(jnp.arange(STREAMS) == chosen, SEQLEN, spread).astype(jnp.int32)


def draw_stamps(key, part):
    anchor = jax.random.randint(key, (STREAMS, 1), 0, 2 ** 20)
    increments = jax.random.randint(jax.random.fold_in(key, 3), (STREAMS, SEQLEN), 0, 64)
    return (anchor + jnp.cumsum(increments, axis=1) - increments[:, :1]).astype(jnp.int32)


def shard_levels(rng, dims, pieces, low, high):
    def one(position, shards_of):
        steps = jax.random.uniform(jax.random.fold_in(jax.random.fold_in(rng, 6), position), (shards_of,), jnp.float32, low / len(pieces), high / len(pieces))
        return jnp.repeat(jnp.exp(steps), dims[position] // shards_of).reshape((-1,) + (1,) * (len(dims) - position - 1))

    loudness = one(*pieces[0])
    for cut in pieces[1:]:
        loudness = loudness * one(*cut)
    return loudness


def normal_values(own_key, shape, deviation, limit, pieces=(), held_as=jnp.bfloat16):
    level = shard_levels(own_key, shape, pieces, -0.22, 0.18) if pieces else 1.0
    entries = jax.random.normal(own_key, shape, jnp.float32) * deviation * level
    return jnp.minimum(jnp.maximum(entries, -limit), limit).astype(held_as)


def setup_inputs(seed: int = 0) -> dict:
    streams_of = jax.random.split(jax.random.key(seed), 10)
    tokens = normal_values(streams_of[0], (STREAMS, SEQLEN, D), 1.0, 6.0, ((0, 8), (1, 4)))
    cotangent = normal_values(streams_of[1], (STREAMS, SEQLEN, D), 1.0, 6.0, ((0, 8), (1, 4)))
    stamps = draw_stamps(jax.random.fold_in(streams_of[9], 71), 0)
    lengths = draw_lengths(jax.random.fold_in(streams_of[9], 71), 0)
    w_qkvu = normal_values(streams_of[4], (D, 4 * D), D ** -0.5, 0.1875, ((0, 8),))
    w_out = normal_values(streams_of[5], (D, D), D ** -0.5, 0.1875, ((0, 8),))
    gain_in = jnp.clip(1.0 + 0.15 * jax.random.normal(streams_of[6], (D,), jnp.float32), 0.25, 1.75)
    gain_out = jnp.clip(1.0 + 0.15 * jax.random.normal(streams_of[7], (D,), jnp.float32), 0.25, 1.75)
    bias_table = normal_values(streams_of[8], (H, NB), 1.0, 4.0, (), jnp.float32)
    return {"tokens": tokens, "cotangent": cotangent, "stamps": stamps, "lengths": lengths, "w_qkvu": w_qkvu, "w_out": w_out, "gain_in": gain_in, "gain_out": gain_out, "bias_table": bias_table}


EPS = 1e-05

def layer_norm(values, gain):
    average = lax.optimization_barrier(jnp.mean(values, axis=-1, keepdims=True))
    centred = values - average
    variance = lax.optimization_barrier(jnp.mean(centred * centred, axis=-1, keepdims=True))
    return centred * lax.rsqrt(variance + EPS) * gain

def silu_slope(values):
    sigmoid_v = jax.nn.sigmoid(values)
    return sigmoid_v * (1.0 + values * (1.0 - sigmoid_v))

def rounded(values):
    return lax.optimization_barrier(values.astype(jnp.bfloat16)).astype(jnp.float32)

def time_bias(bias_table, stamps_q, stamps_k):
    elapsed = stamps_q[:, None] - stamps_k[None, :]
    bucket = jnp.zeros(elapsed.shape, jnp.int32)
    for degree in range(1, bias_table.shape[1]):
        bucket = bucket + (elapsed >= 2 ** degree - 1).astype(jnp.int32)
    biases = jnp.zeros((bias_table.shape[0],) + elapsed.shape, jnp.float32)
    for degree in range(bias_table.shape[1]):
        biases = biases + jnp.where(bucket[None] == degree, bias_table[:, degree][:, None, None], 0.0)
    return biases

def one_stream(x_rows, cot_rows, stamp_row, length, w_qkvu, w_out, gain_in, gain_out, bias_table):
    scale = DH ** (-0.5)
    wide_rows = x_rows.astype(jnp.float32)
    normed = layer_norm(wide_rows, gain_in).astype(jnp.bfloat16)
    projected = jnp.dot(normed, w_qkvu, preferred_element_type=jnp.float32)
    activated = jax.nn.silu(projected)
    gate_u = activated[:, :D]
    v_heads = rounded(activated[:, D:2 * D]).reshape(SEQLEN, H, DH)
    q_heads = rounded(activated[:, 2 * D:3 * D]).reshape(SEQLEN, H, DH)
    k_heads = rounded(activated[:, 3 * D:]).reshape(SEQLEN, H, DH)
    positions = jnp.arange(SEQLEN, dtype=jnp.int32)
    live = positions < length
    allowed = (positions[None, :] <= positions[:, None]) & live[None, :] & live[:, None]
    scores = jnp.einsum('qhd,khd->hqk', q_heads, k_heads) * scale + time_bias(bias_table, stamp_row, stamp_row)
    weight = rounded(jnp.where(allowed[None], jax.nn.silu(scores), 0.0))
    attended = jnp.einsum('hqk,khd->qhd', weight, v_heads).reshape(SEQLEN, D)
    normed_att, norm_back = jax.vjp(lambda values: layer_norm(values, gain_out), attended)
    mixed_rows = (normed_att * gate_u).astype(jnp.bfloat16)
    mixed = (wide_rows + jnp.dot(mixed_rows, w_out, preferred_element_type=jnp.float32)).astype(jnp.bfloat16)
    w_grad = jnp.dot(mixed_rows.T, cot_rows, preferred_element_type=jnp.float32)
    d_mix = jnp.dot(cot_rows, w_out.T, preferred_element_type=jnp.float32)
    d_gate = d_mix * normed_att
    d_heads = rounded(norm_back(d_mix * gate_u)[0]).reshape(SEQLEN, H, DH)
    d_weight = jnp.einsum('qhd,khd->hqk', d_heads, v_heads)
    d_scores = rounded(jnp.where(allowed[None], d_weight * silu_slope(scores), 0.0))
    q_grad = jnp.einsum('hqk,khd->qhd', d_scores, k_heads) * scale
    scores_sh = d_scores.reshape(H, N_SEQ, TOK_DEV, SEQLEN)
    weight_sh = weight.reshape(H, N_SEQ, TOK_DEV, SEQLEN)
    q_sh = q_heads.reshape(N_SEQ, TOK_DEV, H, DH)
    d_sh = d_heads.reshape(N_SEQ, TOK_DEV, H, DH)
    k_parts = rounded(jnp.einsum('hsqk,sqhd->skhd', scores_sh, q_sh) * scale)
    v_parts = rounded(jnp.einsum('hsqk,sqhd->skhd', weight_sh, d_sh))
    k_grad = lax.optimization_barrier(jnp.sum(k_parts, axis=0)).reshape(SEQLEN, D)
    v_grad = lax.optimization_barrier(jnp.sum(v_parts, axis=0)).reshape(SEQLEN, D)
    d_act = jnp.concatenate([d_gate, v_grad, q_grad.reshape(SEQLEN, D), k_grad], axis=1)
    d_proj = (d_act * silu_slope(projected)).astype(jnp.bfloat16)
    d_normed = jnp.dot(d_proj, w_qkvu.T, preferred_element_type=jnp.float32)
    unused_rows, in_back = jax.vjp(lambda values: layer_norm(values, gain_in), wide_rows)
    input_grad = (cot_rows.astype(jnp.float32) + in_back(d_normed)[0]).astype(jnp.bfloat16)
    return (mixed, input_grad, w_grad)

def reference(tokens, cotangent, stamps, lengths, w_qkvu, w_out, gain_in, gain_out, bias_table):

    def visit(total, inputs):
        x_rows, cot_rows, stamp_row, length = inputs
        mixed, input_grad, w_grad = one_stream(x_rows, cot_rows, stamp_row, length, w_qkvu, w_out, gain_in, gain_out, bias_table)
        return (total + w_grad, (mixed, input_grad))
    w_total, outputs = lax.scan(visit, jnp.zeros((D, D), jnp.float32), (tokens, cotangent, stamps, lengths))
    return (outputs[0], outputs[1], w_total)
```

```python
import jax
import jax.numpy as jnp
from jax import lax
from jax.experimental import pallas as pl
from jax.experimental.pallas import tpu as pltpu
from jax.sharding import PartitionSpec as P

H = 8
DH = 128


EPS = 1e-05


def layer_norm(values, gain):
    average = jnp.mean(values, axis=-1, keepdims=True)
    centred = values - average
    variance = jnp.mean(centred * centred, axis=-1, keepdims=True)
    return centred * lax.rsqrt(variance + EPS) * gain


def silu_slope(values):
    sigmoid_v = jax.nn.sigmoid(values)
    return sigmoid_v * (1.0 + values * (1.0 - sigmoid_v))


def time_bias(bias_table, stamps_q, stamps_k):
    elapsed = stamps_q[:, None] - stamps_k[None, :]
    bucket = jnp.zeros(elapsed.shape, jnp.int32)
    for degree in range(1, bias_table.shape[1]):
        bucket = bucket + (elapsed >= 2**degree - 1).astype(jnp.int32)
    levels = jnp.arange(bias_table.shape[1], dtype=jnp.int32)
    one_hot = (bucket[:, :, None] == levels[None, None, :]).astype(jnp.float32)
    return jnp.einsum(
        "qkb,hb->hqk",
        one_hot,
        bias_table,
        precision=lax.Precision.HIGHEST,
        preferred_element_type=jnp.float32,
    )


def pair_terms(
    q_heads, d_heads, stamps_q, pos_q, k_heads, v_heads, stamps_k, pos_k, length, bias_table, scale
):
    scores = (
        jnp.einsum("qhd,khd->hqk", q_heads, k_heads, preferred_element_type=jnp.float32) * scale
    )
    scores = scores + time_bias(bias_table, stamps_q, stamps_k)
    allowed = (
        (pos_k[None, :] <= pos_q[:, None]) & (pos_k[None, :] < length) & (pos_q[:, None] < length)
    )
    weight = jnp.where(allowed[None], jax.nn.silu(scores), 0.0).astype(jnp.bfloat16)
    if d_heads is None:
        return (weight, None)
    d_weight = jnp.einsum("qhd,khd->hqk", d_heads, v_heads, preferred_element_type=jnp.float32)
    d_scores = jnp.where(allowed[None], d_weight * silu_slope(scores), 0.0).astype(jnp.bfloat16)
    return (weight, d_scores)


def per_device(tokens, cotangent, stamps, lengths, w_qkvu, w_out, gain_in, gain_out, bias_table):
    rows = tokens[0]
    cot_rows = cotangent[0]
    tok_count = rows.shape[0]
    feature_width = rows.shape[1]
    seq_count = lax.axis_size("seq")
    total_rows = tok_count * seq_count
    first_row = lax.axis_index("seq") * tok_count
    length = lengths[0]
    stamp_all = stamps[0]
    pos_own = first_row + jnp.arange(tok_count, dtype=jnp.int32)
    stamp_own = lax.dynamic_slice_in_dim(stamp_all, first_row, tok_count)
    scale = DH ** (-0.5)
    block_rows = min(512, total_rows)
    block_count = total_rows // block_rows
    w_full, w_out_full = (
        lax.all_gather(w_qkvu, "dp", axis=0, tiled=True),
        lax.all_gather(w_out, "dp", axis=0, tiled=True),
    )
    wide_rows = rows.astype(jnp.float32)
    normed = layer_norm(wide_rows, gain_in).astype(jnp.bfloat16)
    projected = jnp.dot(normed, w_full, preferred_element_type=jnp.float32)
    activated = jax.nn.silu(projected)
    gate_u = activated[:, :feature_width]
    values_own = activated[:, feature_width : 2 * feature_width].astype(jnp.bfloat16)
    queries_own = activated[:, 2 * feature_width : 3 * feature_width].astype(jnp.bfloat16)
    keys_own = activated[:, 3 * feature_width :].astype(jnp.bfloat16)
    keys_all, values_all = (
        lax.all_gather(keys_own, "seq", axis=0, tiled=True),
        lax.all_gather(values_own, "seq", axis=0, tiled=True),
    )
    q_heads = queries_own.reshape(tok_count, H, DH)

    def key_block(start):
        k_heads = lax.dynamic_slice_in_dim(keys_all, start, block_rows).reshape(block_rows, H, DH)
        v_heads = lax.dynamic_slice_in_dim(values_all, start, block_rows).reshape(block_rows, H, DH)
        stamps_k = lax.dynamic_slice_in_dim(stamp_all, start, block_rows)
        pos_k = start + jnp.arange(block_rows, dtype=jnp.int32)
        return (k_heads, v_heads, stamps_k, pos_k)

    def guarded(active, action, state):
        return lax.cond(active, action, lambda same: same, state)

    def reaches(start):
        return (start <= first_row + tok_count - 1) & (start < length) & (first_row < length)

    def forward_step(block_idx, totals):
        start = block_idx * block_rows

        def forward_compute(totals):
            k_heads, v_heads, stamps_k, pos_k = key_block(start)
            weight, unused = pair_terms(
                q_heads,
                None,
                stamp_own,
                pos_own,
                k_heads,
                v_heads,
                stamps_k,
                pos_k,
                length,
                bias_table,
                scale,
            )
            return totals + jnp.einsum(
                "hqk,khd->qhd", weight, v_heads, preferred_element_type=jnp.float32
            )

        return guarded(reaches(start), forward_compute, totals)

    attended = lax.fori_loop(
        0, block_count, forward_step, jnp.zeros((tok_count, H, DH), jnp.float32)
    )
    attended = attended.reshape(tok_count, feature_width)
    normed_att, norm_back = jax.vjp(lambda values: layer_norm(values, gain_out), attended)
    mixed_rows = (normed_att * gate_u).astype(jnp.bfloat16)
    mixed = (
        wide_rows + jnp.dot(mixed_rows, w_out_full, preferred_element_type=jnp.float32)
    ).astype(jnp.bfloat16)
    grad_part = lax.psum_scatter(
        jnp.einsum("tr,tc->rc", mixed_rows, cot_rows, preferred_element_type=jnp.float32).astype(
            jnp.bfloat16
        ),
        "dp",
        scatter_dimension=0,
        tiled=True,
    )
    w_grad = lax.psum(grad_part, "seq").astype(jnp.float32)
    d_mix = jnp.einsum("tc,rc->tr", cot_rows, w_out_full, preferred_element_type=jnp.float32)
    d_gate = d_mix * normed_att
    d_att = norm_back(d_mix * gate_u)[0].astype(jnp.bfloat16)
    d_heads = d_att.reshape(tok_count, H, DH)

    def backward_step():

        def step(block_idx, state_pair):
            start = block_idx * block_rows

            def step_compute(state_pair):
                q_grad, key_terms = state_pair
                k_heads, v_heads, stamps_k, pos_k = key_block(start)
                weight, d_scores = pair_terms(
                    q_heads,
                    d_heads,
                    stamp_own,
                    pos_own,
                    k_heads,
                    v_heads,
                    stamps_k,
                    pos_k,
                    length,
                    bias_table,
                    scale,
                )
                q_grad = (
                    q_grad
                    + jnp.einsum(
                        "hqk,khd->qhd", d_scores, k_heads, preferred_element_type=jnp.float32
                    )
                    * scale
                )
                k_grad = (
                    jnp.einsum(
                        "hqk,qhd->khd", d_scores, q_heads, preferred_element_type=jnp.float32
                    )
                    * scale
                )
                v_grad = jnp.einsum(
                    "hqk,qhd->khd", weight, d_heads, preferred_element_type=jnp.float32
                )
                joined = jnp.concatenate(
                    [
                        k_grad.reshape(block_rows, feature_width),
                        v_grad.reshape(block_rows, feature_width),
                    ],
                    axis=1,
                )
                key_terms = lax.dynamic_update_slice_in_dim(key_terms, joined, start, 0)
                return (q_grad, key_terms)

            return guarded(reaches(start), step_compute, state_pair)

        return step

    q_start = jnp.zeros((tok_count, H, DH), jnp.float32)
    term_start = jnp.zeros((total_rows, 2 * feature_width), jnp.float32)
    q_grad, key_terms = lax.fori_loop(0, block_count, backward_step(), (q_start, term_start))
    key_grads = lax.psum_scatter(
        key_terms.astype(jnp.bfloat16), "seq", scatter_dimension=0, tiled=True
    ).astype(jnp.float32)
    d_act = jnp.concatenate(
        [
            d_gate,
            key_grads[:, feature_width:],
            q_grad.reshape(tok_count, feature_width),
            key_grads[:, :feature_width],
        ],
        axis=1,
    )
    d_proj = (d_act * silu_slope(projected)).astype(jnp.bfloat16)
    d_normed = jnp.einsum("tf,df->td", d_proj, w_full, preferred_element_type=jnp.float32)
    unused_rows, in_back = jax.vjp(lambda values: layer_norm(values, gain_in), wide_rows)
    input_grad = (cot_rows.astype(jnp.float32) + in_back(d_normed)[0]).astype(jnp.bfloat16)
    return (mixed[None], input_grad[None], w_grad)


MESH = pl.DeviceIdType.MESH
VM = pl.BlockSpec(memory_space=pltpu.VMEM)
F32 = jnp.float32
BF16 = jnp.bfloat16


def plane_of(stream):
    chip, core = stream // 2, stream % 2
    mid = 1 - ((chip + 1) // 2) % 2
    return mid * (1 + core) + (1 - mid) * 3 * core


def plane_sources(plane):
    mid = ((plane + 1) // 2) % 2
    core = mid * (plane - 1) + (1 - mid) * (plane // 3)
    return core, (1 - mid, 2 + mid)


def remote(src, dst, send_sem, recv_sem, target):
    return pltpu.make_async_remote_copy(
        src_ref=src,
        dst_ref=dst,
        send_sem=send_sem,
        recv_sem=recv_sem,
        device_id=target,
        device_id_type=MESH,
    )


def gather_kernel(
    n_dp, n_seq, x_ref, c_ref, w_ref, m_ref, xo_ref, co_ref, wo_ref, mo_ref,
    zsend, fsend, frecv, wsend, wrecv, msend, mrecv, local_sem,
):
    me = lax.axis_index("dp")
    z = lax.axis_index("seq")
    chip, core = me // 2, me % 2
    cy, cx = chip // 2, chip % 2
    x_chip, y_chip = 2 * cy + (1 - cx), 2 * (1 - cy) + cx
    sibling = 2 * chip + (1 - core)
    rows = w_ref.shape[0]
    width = x_ref.shape[1]
    home = plane_of(me)
    slot = chip // 2
    src_core, chips = plane_sources(z)
    ins, outs = (x_ref, c_ref), (xo_ref, co_ref)

    def z_send(a, s):
        return remote(ins[a], outs[a].at[slot, s], zsend.at[a], frecv.at[a, slot, s], (me, home))

    def own_copy(a):
        return pltpu.make_async_copy(ins[a], outs[a].at[slot, z], local_sem.at[a])

    def w_send(peer, group):
        return remote(
            w_ref.at[:, pl.ds(pl.multiple_of(group * width + peer * DH, DH), DH)],
            wo_ref.at[pl.ds(pl.multiple_of(me * rows, rows), rows), pl.ds(group * DH, DH)],
            wsend.at[peer, group],
            wrecv.at[me, group],
            (peer, z),
        )

    def w_arrive(peer, group):
        return remote(
            w_ref.at[:, pl.ds(pl.multiple_of(group * width + me * DH, DH), DH)],
            wo_ref.at[pl.ds(pl.multiple_of(peer * rows, rows), rows), pl.ds(group * DH, DH)],
            wsend.at[peer, group],
            wrecv.at[peer, group],
            (peer, z),
        )

    def w_own(group):
        return pltpu.make_async_copy(
            w_ref.at[:, pl.ds(pl.multiple_of(group * width + me * DH, DH), DH)],
            wo_ref.at[pl.ds(pl.multiple_of(me * rows, rows), rows), pl.ds(group * DH, DH)],
            local_sem.at[3 + group],
        )

    def m_send(peer):
        return remote(m_ref, mo_ref.at[slot], msend.at[peer], mrecv.at[slot], (peer, z))

    def m_own():
        return pltpu.make_async_copy(m_ref, mo_ref.at[slot], local_sem.at[2])

    @pl.when(home != z)
    def _():
        z_send(0, z).start()

    @pl.when(home == z)
    def _():
        own_copy(0).start()
        m_own().start()

    for step in range(1, n_dp):
        peer = lax.rem(me + step, n_dp)

        @pl.when(home == z)
        def _():
            m_send(peer).start()

        for group in range(4):
            w_send(peer, group).start()
    for group in range(4):
        w_own(group).start()

    @pl.when(home != z)
    def _():
        z_send(1, z).start()

    @pl.when(home == z)
    def _():
        own_copy(1).start()

    def forwards(a, j, b):
        block = outs[a].at[j, b]
        owner = chips[j]
        mine = core == src_core

        def to(target, leg):
            return remote(block, block, fsend.at[a, j, b, leg], frecv.at[a, j, b], (target, z))

        via_y = (chip == owner) | ((x_chip == owner) & (b < n_seq // 2))
        via_x = (chip == owner) | ((y_chip == owner) & (b >= n_seq // 2))
        return (
            (mine & via_x, to(2 * x_chip + core, 0)),
            (mine & via_y, to(2 * y_chip + core, 1)),
            (mine, to(sibling, 2)),
        )

    for a in range(2):
        for b in range(n_seq):
            for j in range(2):
                block = outs[a].at[j, b]
                held = (me == 2 * chips[j] + src_core) & (z == b)

                @pl.when(held)
                def _():
                    own_copy(a).wait()

                @pl.when(jnp.logical_not(held))
                def _():
                    remote(block, block, zsend.at[a], frecv.at[a, j, b], (me, z)).wait_recv()

                for use, copy in forwards(a, j, b):

                    @pl.when(use)
                    def _():
                        copy.start()

    for step in range(1, n_dp):
        peer = lax.rem(me + step, n_dp)
        for group in range(4):
            w_arrive(peer, group).wait_recv()
            w_send(peer, group).wait_send()

        @pl.when(home == z)
        def _():
            m_send(peer).wait_send()

    for group in range(4):
        w_own(group).wait()

    @pl.when(home == z)
    def _():
        m_own().wait()

    for j in range(2):

        @pl.when(jnp.logical_not((home == z) & (slot == j)))
        def _():
            remote(m_ref, mo_ref.at[j], msend.at[0], mrecv.at[j], (me, z)).wait_recv()

    for a in range(2):

        @pl.when(home != z)
        def _():
            z_send(a, z).wait_send()

        for b in range(n_seq):
            for j in range(2):
                for use, copy in forwards(a, j, b):

                    @pl.when(use)
                    def _():
                        copy.wait_send()


def stats_kernel(n_dp, s_ref, o_ref, send, recv, local_sem):
    me = lax.axis_index("dp")
    z = lax.axis_index("seq")
    own = pltpu.make_async_copy(s_ref, o_ref.at[me], local_sem)
    own.start()
    for step in range(1, n_dp):
        peer = lax.rem(me + step, n_dp)
        remote(s_ref, o_ref.at[me], send.at[peer], recv.at[me], (peer, z)).start()
    own.wait()
    for step in range(1, n_dp):
        peer = lax.rem(me + step, n_dp)
        copy = remote(s_ref, o_ref.at[peer], send.at[peer], recv.at[peer], (peer, z))
        copy.wait_recv()
        copy.wait_send()


def reduce_kernel(
    n_dp, n_seq, p_ref, g_ref, o_ref, go_ref, pair, mixed_up, landed, final, g_land, g_sum,
    psend, precv, csend, crecv, osend, orecv, gsend, grecv, hsend, hrecv, local_sem,
):
    me = lax.axis_index("dp")
    z = lax.axis_index("seq")
    chip, core = me // 2, me % 2
    sibling = 2 * chip + (1 - core)
    chips_n = n_dp // 2
    g_rows = g_ref.shape[0] // n_seq

    def g_slice(ref, index):
        return ref.at[pl.ds(pl.multiple_of(index * g_rows, g_rows), g_rows)]

    def pair_send(part, c):
        return remote(
            p_ref.at[part, 2 * c + (1 - core)], pair.at[part, c],
            psend.at[part, c], precv.at[part, c], (sibling, z),
        )

    def cross_send(part, c):
        return remote(
            mixed_up.at[part, c], landed.at[part, chip],
            csend.at[part, c], crecv.at[part, chip], (2 * c + core, z),
        )

    def cross_arrive(part, c):
        return remote(
            mixed_up.at[part, c], landed.at[part, c],
            csend.at[part, c], crecv.at[part, c], (2 * c + core, z),
        )

    def g_send(peer):
        return remote(
            g_slice(g_ref, peer), g_land.at[z], gsend.at[peer], grecv.at[z], (me, peer)
        )

    def g_arrive(peer):
        return remote(
            g_slice(g_ref, peer), g_land.at[peer], gsend.at[peer], grecv.at[peer], (me, peer)
        )

    def h_send(peer):
        return remote(g_sum, g_slice(go_ref, z), hsend.at[peer], hrecv.at[z], (me, peer))

    def h_arrive(peer):
        return remote(g_sum, g_slice(go_ref, peer), hsend.at[peer], hrecv.at[peer], (me, peer))

    others = [lax.rem(chip + step, chips_n) for step in range(1, chips_n)]
    peers = [lax.rem(z + step, n_seq) for step in range(1, n_seq)]
    parts = p_ref.shape[0]
    for part in range(parts):
        for c in others + [chip]:
            pair_send(part, c).start()
    for peer in peers:
        g_send(peer).start()
    for part in range(parts):
        for c in others + [chip]:
            pair_send(part, c).wait_recv()
            mixed_up[part, c] = (
                p_ref[part, 2 * c + core].astype(F32) + pair[part, c].astype(F32)
            ).astype(BF16)
            if c is not chip:
                cross_send(part, c).start()
    total = g_slice(g_ref, z)[...].astype(F32)
    for peer in peers:
        g_arrive(peer).wait_recv()
        total = total + g_land[peer].astype(F32)
    g_sum[...] = total.astype(BF16)
    own_g = pltpu.make_async_copy(g_sum, g_slice(go_ref, z), local_sem.at[0])
    own_g.start()
    for peer in peers:
        h_send(peer).start()
    block, half = me % n_seq, me // n_seq
    src_core, sources = plane_sources(z)
    stream = 2 * ((1 - half) * sources[0] + half * sources[1]) + src_core
    stays = (stream == me) & (block == z)
    gone = jnp.logical_not(stays)
    home = plane_of(me)
    from_dp = (chip // 2) * n_seq + z
    arrives = jnp.logical_not((home == z) & (from_dp == me))

    def final_send(part):
        return remote(
            final.at[part], o_ref.at[part], osend.at[part], orecv.at[part], (stream, block)
        )

    def final_own(part):
        return pltpu.make_async_copy(final.at[part], o_ref.at[part], local_sem.at[1 + part])

    for part in range(parts):
        total = mixed_up[part, chip].astype(F32)
        for c in others:
            cross_arrive(part, c).wait_recv()
            total = total + landed[part, c].astype(F32)
        final[part] = total.astype(BF16)

        @pl.when(gone)
        def _():
            final_send(part).start()

        @pl.when(stays)
        def _():
            final_own(part).start()

    for part in range(parts):
        for c in others + [chip]:
            pair_send(part, c).wait_send()
        for c in others:
            cross_send(part, c).wait_send()

        @pl.when(gone)
        def _():
            final_send(part).wait_send()

        @pl.when(stays)
        def _():
            final_own(part).wait()

        @pl.when(arrives)
        def _():
            final_send(part).wait_recv()

    own_g.wait()
    for peer in peers:
        g_send(peer).wait_send()
        h_send(peer).wait_send()
        h_arrive(peer).wait_recv()


def mm(a, b, dims):
    return lax.dot_general(a, b, (dims, ((), ())), preferred_element_type=F32)


def forward_kernel(
    bias_ref, len_ref, proj_ref, srow_ref, scol_ref, att_ref, weight_ref, slope_ref
):
    length = len_ref[pl.program_id(0)]
    head = lax.axis_index("dp")
    total = proj_ref.shape[1]
    rows = total // 4
    acts = [jax.nn.silu(proj_ref[0, :, (1 + g) * DH : (2 + g) * DH]).astype(BF16) for g in range(3)]
    values, queries, keys = acts
    for start in range(0, total, rows):
        end = start + rows
        scores = mm(queries[start:end], keys[:end], ((1,), (1,))) * DH ** (-0.5)
        elapsed = scol_ref[0, start:end, :] - srow_ref[0, :, :end]
        bias = jnp.full(elapsed.shape, bias_ref[head, 0], F32)
        for degree in range(1, bias_ref.shape[1]):
            bias = jnp.where(elapsed >= 2**degree - 1, bias_ref[head, degree], bias)
        scores = scores + bias
        pos_q = start + lax.broadcasted_iota(jnp.int32, elapsed.shape, 0)
        pos_k = lax.broadcasted_iota(jnp.int32, elapsed.shape, 1)
        allowed = (pos_k <= pos_q) & (pos_k < length) & (pos_q < length)
        sig = jax.nn.sigmoid(scores)
        weight = jnp.where(allowed, scores * sig, 0.0).astype(BF16)
        weight_ref[0, start:end, :end] = weight
        slope_ref[0, start:end, :end] = jnp.where(allowed, sig * (1.0 + scores * (1.0 - sig)), 0.0)
        att_ref[0, start:end, :] = mm(weight, values[:end], ((1,), (0,)))


def backward_kernel(proj_ref, datt_ref, dgate_ref, weight_ref, slope_ref, out_ref, k_acc, v_acc):
    total = proj_ref.shape[1]
    rows = total // 4
    acts = [jax.nn.silu(proj_ref[0, :, (1 + g) * DH : (2 + g) * DH]).astype(BF16) for g in range(3)]
    values, queries, keys = acts
    scale = DH ** (-0.5)

    def put(group, start, end, grad):
        cols = slice(group * DH, (group + 1) * DH)
        out_ref[0, start:end, cols] = (grad * silu_slope(proj_ref[0, start:end, cols])).astype(BF16)

    for start in reversed(range(0, total, rows)):
        end = start + rows
        d_att = datt_ref[0, start:end, :]
        d_weight = mm(d_att, values[:end], ((1,), (1,)))
        d_scores = (d_weight * slope_ref[0, start:end, :end]).astype(BF16)
        put(2, start, end, mm(d_scores, keys[:end], ((1,), (0,))) * scale)
        k_part = mm(d_scores, queries[start:end], ((0,), (0,)))
        v_part = mm(weight_ref[0, start:end, :end], d_att, ((0,), (0,)))
        if end == total:
            k_acc[...] = k_part
            v_acc[...] = v_part
        else:
            k_acc[:end] += k_part
            v_acc[:end] += v_part
    put(0, 0, total, dgate_ref[0])
    put(1, 0, total, v_acc[...])
    put(3, 0, total, k_acc[...] * scale)


def head_parallel(
    n_dp, n_seq, tokens, cotangent, stamps, lengths, w_qkvu, w_out, gain_in, gain_out, bias_table
):
    tok, width = tokens.shape[1:]
    seq_len = stamps.shape[1]
    head = lax.axis_index("dp")
    meta = jnp.concatenate([stamps.reshape(-1, DH), jnp.broadcast_to(lengths[:, None], (4, DH))])
    dma = pltpu.SemaphoreType.DMA
    sds = jax.ShapeDtypeStruct
    side = pltpu.CompilerParams(has_side_effects=True)
    x_all, c_all, w_head, metas = pl.pallas_call(
        lambda *refs: gather_kernel(n_dp, n_seq, *refs),
        out_shape=(
            sds((2, n_seq, tok, width), BF16),
            sds((2, n_seq, tok, width), BF16),
            sds((width, 4 * DH), BF16),
            sds((2,) + meta.shape, jnp.int32),
        ),
        in_specs=[VM] * 4,
        out_specs=[VM] * 4,
        scratch_shapes=[
            dma((2,)),
            dma((2, 2, n_seq, 3)),
            dma((2, 2, n_seq)),
            dma((n_dp, 4)),
            dma((n_dp, 4)),
            dma((n_dp,)),
            dma((2,)),
            dma((7,)),
        ],
        compiler_params=side,
        name="gather",
    )(tokens[0], cotangent[0], w_qkvu, meta)
    count = 2 * seq_len
    x_rows = x_all.reshape(count, width)
    c_rows = c_all.reshape(count, width)
    stamp_rows = metas[:, : seq_len // DH].reshape(2, 1, seq_len)
    stamp_cols = stamp_rows.reshape(2, seq_len, 1)
    spans = metas[:, seq_len // DH, 0]
    normed = layer_norm(x_rows.astype(F32), gain_in).astype(BF16)
    projected = jnp.dot(normed, w_head, preferred_element_type=F32)
    proj3 = projected.reshape(2, seq_len, 4 * DH)
    smem = pl.BlockSpec(memory_space=pltpu.SMEM)

    def per(*shape):
        return pl.BlockSpec((1,) + shape, lambda i: (i,) + (0,) * len(shape))

    attended, weight, slope = pl.pallas_call(
        forward_kernel,
        grid=(2,),
        out_shape=(
            sds((2, seq_len, DH), F32),
            sds((2, seq_len, seq_len), BF16),
            sds((2, seq_len, seq_len), F32),
        ),
        in_specs=[smem, smem, per(seq_len, 4 * DH), per(1, seq_len), per(seq_len, 1)],
        out_specs=[per(seq_len, DH), per(seq_len, seq_len), per(seq_len, seq_len)],
        name="forward",
    )(bias_table, spans, proj3, stamp_rows, stamp_cols)
    att = attended.reshape(count, DH)
    gate = jax.nn.silu(projected[:, :DH])
    gain_head = lax.dynamic_slice_in_dim(gain_out, head * DH, DH)
    d_mix = lax.dot_general(c_rows, w_out, (((1,), (1,)), ((), ())), preferred_element_type=F32)
    g = d_mix * gate * gain_head
    mean_own = jnp.mean(att, axis=1)
    off = att - mean_own[:, None]
    stats = jnp.stack(
        [mean_own, jnp.sum(off * off, axis=1), jnp.sum(g, axis=1), jnp.sum(g * off, axis=1)]
    )
    gathered = pl.pallas_call(
        lambda *refs: stats_kernel(n_dp, *refs),
        out_shape=sds((n_dp, 4, count // DH, DH), F32),
        in_specs=[VM],
        out_specs=VM,
        scratch_shapes=[dma((n_dp,)), dma((n_dp,)), dma],
        compiler_params=side,
        name="stats",
    )(stats.reshape(4, count // DH, DH))
    means, squares, g_sums, g_offs = [gathered[:, k] for k in range(4)]
    mean = jnp.mean(means, axis=0)
    shift = means - mean[None]
    variance = jnp.sum(squares + DH * shift * shift, axis=0) / width
    rstd = lax.rsqrt(variance + EPS)
    g_mean = jnp.sum(g_sums, axis=0) / width
    g_dot = rstd * jnp.sum(g_offs + shift * g_sums, axis=0) / width
    mean, rstd, g_mean, g_dot = [v.reshape(count, 1) for v in (mean, rstd, g_mean, g_dot)]
    hat = (att - mean) * rstd
    normed_att = hat * gain_head
    mixed_rows = (normed_att * gate).astype(BF16)
    d_gate = d_mix * normed_att
    d_att = (rstd * (g - g_mean - hat * g_dot)).astype(BF16)
    d_proj = pl.pallas_call(
        backward_kernel,
        grid=(2,),
        out_shape=sds((2, seq_len, 4 * DH), BF16),
        in_specs=[
            per(seq_len, 4 * DH),
            per(seq_len, DH),
            per(seq_len, DH),
            per(seq_len, seq_len),
            per(seq_len, seq_len),
        ],
        out_specs=per(seq_len, 4 * DH),
        scratch_shapes=[pltpu.VMEM((seq_len, DH), F32)] * 2,
        name="backward",
    )(proj3, d_att.reshape(2, seq_len, DH), d_gate.reshape(2, seq_len, DH), weight, slope)
    mixed_part = jnp.dot(mixed_rows, w_out, preferred_element_type=F32).astype(BF16)
    d_part = lax.dot_general(
        d_proj.reshape(count, 4 * DH), w_head, (((1,), (1,)), ((), ())), preferred_element_type=F32
    ).astype(BF16)
    w_part = lax.dot_general(
        mixed_rows, c_rows, (((0,), (0,)), ((), ())), preferred_element_type=F32
    ).astype(BF16)
    shape = (n_dp, tok, width)
    half = n_dp // 2
    sums, w_sum = pl.pallas_call(
        lambda *refs: reduce_kernel(n_dp, n_seq, *refs),
        out_shape=(sds((2, tok, width), BF16), sds(w_part.shape, BF16)),
        in_specs=[VM] * 2,
        out_specs=[VM] * 2,
        scratch_shapes=[
            pltpu.VMEM((2, half, tok, width), BF16),
            pltpu.VMEM((2, half, tok, width), BF16),
            pltpu.VMEM((2, half, tok, width), BF16),
            pltpu.VMEM((2, tok, width), BF16),
            pltpu.VMEM((n_seq, w_part.shape[0] // n_seq, width), BF16),
            pltpu.VMEM((w_part.shape[0] // n_seq, width), BF16),
            dma((2, half)),
            dma((2, half)),
            dma((2, half)),
            dma((2, half)),
            dma((2,)),
            dma((2,)),
            dma((n_seq,)),
            dma((n_seq,)),
            dma((n_seq,)),
            dma((n_seq,)),
            dma((3,)),
        ],
        compiler_params=side,
        name="reduce",
    )(jnp.stack([mixed_part.reshape(shape), d_part.reshape(shape)]), w_part)
    wide_rows = tokens[0].astype(F32)
    mixed = (wide_rows + sums[0].astype(F32)).astype(BF16)
    unused_rows, in_back = jax.vjp(lambda values: layer_norm(values, gain_in), wide_rows)
    back = in_back(sums[1].astype(F32))[0]
    input_grad = (cotangent[0].astype(F32) + back).astype(BF16)
    return (mixed[None], input_grad[None], w_sum.astype(F32))


def solution(mesh):
    n_dp, n_seq = mesh.shape["dp"], mesh.shape["seq"]

    def body(*args):
        streams_fit = n_dp == 2 * n_seq and n_dp == H and args[5].shape[0] == DH
        if streams_fit and args[2].shape[0] == 1:
            return head_parallel(n_dp, n_seq, *args)
        return per_device(*args)

    return jax.shard_map(
        body,
        mesh=mesh,
        in_specs=(
            P("dp", "seq", None),
            P("dp", "seq", None),
            P("dp", None),
            P("dp"),
            P("dp", None),
            P("dp", None),
            P(),
            P(),
            P(),
        ),
        out_specs=(P("dp", "seq", None), P("dp", "seq", None), P("dp", None)),
        check_vma=False,
    )
```

```python
import jax
import jax.numpy as jnp
from jax import lax
from jax.experimental import pallas as pl
from jax.experimental.pallas import tpu as pltpu
from jax.sharding import PartitionSpec as P

H = 8
DH = 128


EPS = 1e-05


def layer_norm(values, gain):
    average = jnp.mean(values, axis=-1, keepdims=True)
    centred = values - average
    variance = jnp.mean(centred * centred, axis=-1, keepdims=True)
    return centred * lax.rsqrt(variance + EPS) * gain


def silu_slope(values):
    sigmoid_v = jax.nn.sigmoid(values)
    return sigmoid_v * (1.0 + values * (1.0 - sigmoid_v))


def time_bias(bias_table, stamps_q, stamps_k):
    elapsed = stamps_q[:, None] - stamps_k[None, :]
    bucket = jnp.zeros(elapsed.shape, jnp.int32)
    for degree in range(1, bias_table.shape[1]):
        bucket = bucket + (elapsed >= 2**degree - 1).astype(jnp.int32)
    levels = jnp.arange(bias_table.shape[1], dtype=jnp.int32)
    one_hot = (bucket[:, :, None] == levels[None, None, :]).astype(jnp.float32)
    return jnp.einsum(
        "qkb,hb->hqk",
        one_hot,
        bias_table,
        precision=lax.Precision.HIGHEST,
        preferred_element_type=jnp.float32,
    )


def pair_terms(
    q_heads, d_heads, stamps_q, pos_q, k_heads, v_heads, stamps_k, pos_k, length, bias_table, scale
):
    scores = (
        jnp.einsum("qhd,khd->hqk", q_heads, k_heads, preferred_element_type=jnp.float32) * scale
    )
    scores = scores + time_bias(bias_table, stamps_q, stamps_k)
    allowed = (
        (pos_k[None, :] <= pos_q[:, None]) & (pos_k[None, :] < length) & (pos_q[:, None] < length)
    )
    weight = jnp.where(allowed[None], jax.nn.silu(scores), 0.0).astype(jnp.bfloat16)
    if d_heads is None:
        return (weight, None)
    d_weight = jnp.einsum("qhd,khd->hqk", d_heads, v_heads, preferred_element_type=jnp.float32)
    d_scores = jnp.where(allowed[None], d_weight * silu_slope(scores), 0.0).astype(jnp.bfloat16)
    return (weight, d_scores)


def per_device(tokens, cotangent, stamps, lengths, w_qkvu, w_out, gain_in, gain_out, bias_table):
    rows = tokens[0]
    cot_rows = cotangent[0]
    tok_count = rows.shape[0]
    feature_width = rows.shape[1]
    seq_count = lax.axis_size("seq")
    total_rows = tok_count * seq_count
    first_row = lax.axis_index("seq") * tok_count
    length = lengths[0]
    stamp_all = stamps[0]
    pos_own = first_row + jnp.arange(tok_count, dtype=jnp.int32)
    stamp_own = lax.dynamic_slice_in_dim(stamp_all, first_row, tok_count)
    scale = DH ** (-0.5)
    block_rows = min(512, total_rows)
    block_count = total_rows // block_rows
    w_full, w_out_full = (
        lax.all_gather(w_qkvu, "dp", axis=0, tiled=True),
        lax.all_gather(w_out, "dp", axis=0, tiled=True),
    )
    wide_rows = rows.astype(jnp.float32)
    normed = layer_norm(wide_rows, gain_in).astype(jnp.bfloat16)
    projected = jnp.dot(normed, w_full, preferred_element_type=jnp.float32)
    activated = jax.nn.silu(projected)
    gate_u = activated[:, :feature_width]
    values_own = activated[:, feature_width : 2 * feature_width].astype(jnp.bfloat16)
    queries_own = activated[:, 2 * feature_width : 3 * feature_width].astype(jnp.bfloat16)
    keys_own = activated[:, 3 * feature_width :].astype(jnp.bfloat16)
    keys_all, values_all = (
        lax.all_gather(keys_own, "seq", axis=0, tiled=True),
        lax.all_gather(values_own, "seq", axis=0, tiled=True),
    )
    q_heads = queries_own.reshape(tok_count, H, DH)

    def key_block(start):
        k_heads = lax.dynamic_slice_in_dim(keys_all, start, block_rows).reshape(block_rows, H, DH)
        v_heads = lax.dynamic_slice_in_dim(values_all, start, block_rows).reshape(block_rows, H, DH)
        stamps_k = lax.dynamic_slice_in_dim(stamp_all, start, block_rows)
        pos_k = start + jnp.arange(block_rows, dtype=jnp.int32)
        return (k_heads, v_heads, stamps_k, pos_k)

    def guarded(active, action, state):
        return lax.cond(active, action, lambda same: same, state)

    def reaches(start):
        return (start <= first_row + tok_count - 1) & (start < length) & (first_row < length)

    def forward_step(block_idx, totals):
        start = block_idx * block_rows

        def forward_compute(totals):
            k_heads, v_heads, stamps_k, pos_k = key_block(start)
            weight, unused = pair_terms(
                q_heads,
                None,
                stamp_own,
                pos_own,
                k_heads,
                v_heads,
                stamps_k,
                pos_k,
                length,
                bias_table,
                scale,
            )
            return totals + jnp.einsum(
                "hqk,khd->qhd", weight, v_heads, preferred_element_type=jnp.float32
            )

        return guarded(reaches(start), forward_compute, totals)

    attended = lax.fori_loop(
        0, block_count, forward_step, jnp.zeros((tok_count, H, DH), jnp.float32)
    )
    attended = attended.reshape(tok_count, feature_width)
    normed_att, norm_back = jax.vjp(lambda values: layer_norm(values, gain_out), attended)
    mixed_rows = (normed_att * gate_u).astype(jnp.bfloat16)
    mixed = (
        wide_rows + jnp.dot(mixed_rows, w_out_full, preferred_element_type=jnp.float32)
    ).astype(jnp.bfloat16)
    grad_part = lax.psum_scatter(
        jnp.einsum("tr,tc->rc", mixed_rows, cot_rows, preferred_element_type=jnp.float32).astype(
            jnp.bfloat16
        ),
        "dp",
        scatter_dimension=0,
        tiled=True,
    )
    w_grad = lax.psum(grad_part, "seq").astype(jnp.float32)
    d_mix = jnp.einsum("tc,rc->tr", cot_rows, w_out_full, preferred_element_type=jnp.float32)
    d_gate = d_mix * normed_att
    d_att = norm_back(d_mix * gate_u)[0].astype(jnp.bfloat16)
    d_heads = d_att.reshape(tok_count, H, DH)

    def backward_step():

        def step(block_idx, state_pair):
            start = block_idx * block_rows

            def step_compute(state_pair):
                q_grad, key_terms = state_pair
                k_heads, v_heads, stamps_k, pos_k = key_block(start)
                weight, d_scores = pair_terms(
                    q_heads,
                    d_heads,
                    stamp_own,
                    pos_own,
                    k_heads,
                    v_heads,
                    stamps_k,
                    pos_k,
                    length,
                    bias_table,
                    scale,
                )
                q_grad = (
                    q_grad
                    + jnp.einsum(
                        "hqk,khd->qhd", d_scores, k_heads, preferred_element_type=jnp.float32
                    )
                    * scale
                )
                k_grad = (
                    jnp.einsum(
                        "hqk,qhd->khd", d_scores, q_heads, preferred_element_type=jnp.float32
                    )
                    * scale
                )
                v_grad = jnp.einsum(
                    "hqk,qhd->khd", weight, d_heads, preferred_element_type=jnp.float32
                )
                joined = jnp.concatenate(
                    [
                        k_grad.reshape(block_rows, feature_width),
                        v_grad.reshape(block_rows, feature_width),
                    ],
                    axis=1,
                )
                key_terms = lax.dynamic_update_slice_in_dim(key_terms, joined, start, 0)
                return (q_grad, key_terms)

            return guarded(reaches(start), step_compute, state_pair)

        return step

    q_start = jnp.zeros((tok_count, H, DH), jnp.float32)
    term_start = jnp.zeros((total_rows, 2 * feature_width), jnp.float32)
    q_grad, key_terms = lax.fori_loop(0, block_count, backward_step(), (q_start, term_start))
    key_grads = lax.psum_scatter(
        key_terms.astype(jnp.bfloat16), "seq", scatter_dimension=0, tiled=True
    ).astype(jnp.float32)
    d_act = jnp.concatenate(
        [
            d_gate,
            key_grads[:, feature_width:],
            q_grad.reshape(tok_count, feature_width),
            key_grads[:, :feature_width],
        ],
        axis=1,
    )
    d_proj = (d_act * silu_slope(projected)).astype(jnp.bfloat16)
    d_normed = jnp.einsum("tf,df->td", d_proj, w_full, preferred_element_type=jnp.float32)
    unused_rows, in_back = jax.vjp(lambda values: layer_norm(values, gain_in), wide_rows)
    input_grad = (cot_rows.astype(jnp.float32) + in_back(d_normed)[0]).astype(jnp.bfloat16)
    return (mixed[None], input_grad[None], w_grad)


MESH = pl.DeviceIdType.MESH
VM = pl.BlockSpec(memory_space=pltpu.VMEM)
F32 = jnp.float32
BF16 = jnp.bfloat16


def plane_of(stream):
    chip, core = stream // 2, stream % 2
    mid = 1 - ((chip + 1) // 2) % 2
    return mid * (1 + core) + (1 - mid) * 3 * core


def plane_sources(plane):
    mid = ((plane + 1) // 2) % 2
    core = mid * (plane - 1) + (1 - mid) * (plane // 3)
    return core, (1 - mid, 2 + mid)


def remote(src, dst, send_sem, recv_sem, target):
    return pltpu.make_async_remote_copy(
        src_ref=src,
        dst_ref=dst,
        send_sem=send_sem,
        recv_sem=recv_sem,
        device_id=target,
        device_id_type=MESH,
    )


def gather_kernel(
    n_dp, n_seq, x_ref, c_ref, w_ref, m_ref, xo_ref, co_ref, wo_ref, mo_ref,
    zsend, fsend, frecv, wsend, wrecv, msend, mrecv, local_sem,
):
    me = lax.axis_index("dp")
    z = lax.axis_index("seq")
    chip, core = me // 2, me % 2
    cy, cx = chip // 2, chip % 2
    x_chip, y_chip = 2 * cy + (1 - cx), 2 * (1 - cy) + cx
    sibling = 2 * chip + (1 - core)
    home = plane_of(me)
    slot = chip // 2
    src_core, chips = plane_sources(z)
    ins, outs = (x_ref, c_ref), (xo_ref, co_ref)

    def z_send(a, s):
        return remote(ins[a], outs[a].at[slot, s], zsend.at[a], frecv.at[a, slot, s], (me, home))

    def own_copy(a):
        return pltpu.make_async_copy(ins[a], outs[a].at[slot, z], local_sem.at[a])

    def w_send(peer):
        return remote(w_ref.at[peer], wo_ref.at[me], wsend.at[peer], wrecv.at[me], (peer, z))

    def w_arrive(peer):
        return remote(w_ref.at[peer], wo_ref.at[peer], wsend.at[peer], wrecv.at[peer], (peer, z))

    def w_own():
        return pltpu.make_async_copy(w_ref.at[me], wo_ref.at[me], local_sem.at[3])

    def m_send(peer):
        return remote(m_ref, mo_ref.at[slot], msend.at[peer], mrecv.at[slot], (peer, z))

    def m_own():
        return pltpu.make_async_copy(m_ref, mo_ref.at[slot], local_sem.at[2])

    @pl.when(home != z)
    def _():
        z_send(0, z).start()

    @pl.when(home == z)
    def _():
        own_copy(0).start()
        m_own().start()

    for step in range(1, n_dp):
        peer = lax.rem(me + step, n_dp)

        @pl.when(home == z)
        def _():
            m_send(peer).start()

        w_send(peer).start()
    w_own().start()

    @pl.when(home != z)
    def _():
        z_send(1, z).start()

    @pl.when(home == z)
    def _():
        own_copy(1).start()

    def order(i):
        return lax.rem(z + i, n_seq)

    def pass_on(a, j, b, target, leg):
        block = outs[a].at[j, b]
        return remote(block, block, fsend.at[a, j, b, leg], frecv.at[a, j, b], (target, z))

    def from_source(a, i):
        b = order(i)
        return (
            pass_on(a, slot, b, 2 * x_chip + core, 0),
            pass_on(a, slot, b, 2 * y_chip + core, 1),
            pass_on(a, slot, b, sibling, 2),
        )

    is_source = home == z
    relays = core == src_core

    def relayed(a, i, j):
        b = order(i)
        if i % 2 == 0:
            return relays & (x_chip == chips[j]), pass_on(a, j, b, 2 * y_chip + core, 1)
        return relays & (y_chip == chips[j]), pass_on(a, j, b, 2 * x_chip + core, 0)

    def shared(a, i, j):
        return relays & (chip != chips[j]), pass_on(a, j, order(i), sibling, 2)

    for a in range(2):

        @pl.when(is_source)
        def _():
            for i in range(n_seq):
                if i == 0:
                    own_copy(a).wait()
                else:
                    pass_on(a, slot, order(i), me, 0).wait_recv()
                for copy in from_source(a, i):
                    copy.start()

    for a in range(2):
        for i in range(n_seq):
            for j in range(2):

                @pl.when(jnp.logical_not(is_source & (slot == j)))
                def _():
                    pass_on(a, j, order(i), me, 0).wait_recv()

                for use, copy in (relayed(a, i, j), shared(a, i, j)):

                    @pl.when(use)
                    def _():
                        copy.start()

    for step in range(1, n_dp):
        peer = lax.rem(me + step, n_dp)
        w_arrive(peer).wait_recv()
        w_send(peer).wait_send()

        @pl.when(home == z)
        def _():
            m_send(peer).wait_send()

    w_own().wait()

    @pl.when(home == z)
    def _():
        m_own().wait()

    for j in range(2):

        @pl.when(jnp.logical_not((home == z) & (slot == j)))
        def _():
            remote(m_ref, mo_ref.at[j], msend.at[0], mrecv.at[j], (me, z)).wait_recv()

    for a in range(2):

        @pl.when(home != z)
        def _():
            z_send(a, z).wait_send()

        @pl.when(is_source)
        def _():
            for i in range(n_seq):
                for copy in from_source(a, i):
                    copy.wait_send()

        for i in range(n_seq):
            for j in range(2):
                for use, copy in (relayed(a, i, j), shared(a, i, j)):

                    @pl.when(use)
                    def _():
                        copy.wait_send()


def stats_kernel(n_dp, s_ref, o_ref, send, recv, local_sem):
    me = lax.axis_index("dp")
    z = lax.axis_index("seq")
    own = pltpu.make_async_copy(s_ref, o_ref.at[me], local_sem)
    own.start()
    for step in range(1, n_dp):
        peer = lax.rem(me + step, n_dp)
        remote(s_ref, o_ref.at[me], send.at[peer], recv.at[me], (peer, z)).start()
    own.wait()
    for step in range(1, n_dp):
        peer = lax.rem(me + step, n_dp)
        copy = remote(s_ref, o_ref.at[peer], send.at[peer], recv.at[peer], (peer, z))
        copy.wait_recv()
        copy.wait_send()


def reduce_kernel(
    n_dp, n_seq, p_ref, g_ref, o_ref, go_ref, pair, mixed_up, landed, final, g_land, g_sum,
    psend, precv, csend, crecv, osend, orecv, gsend, grecv, hsend, hrecv, local_sem,
):
    me = lax.axis_index("dp")
    z = lax.axis_index("seq")
    chip, core = me // 2, me % 2
    sibling = 2 * chip + (1 - core)
    chips_n = n_dp // 2
    g_rows = g_ref.shape[0] // n_seq

    def g_slice(ref, index):
        return ref.at[pl.ds(pl.multiple_of(index * g_rows, g_rows), g_rows)]

    def pair_send(part, c):
        return remote(
            p_ref.at[part, 2 * c + (1 - core)], pair.at[part, c],
            psend.at[part, c], precv.at[part, c], (sibling, z),
        )

    def cross_send(part, c):
        return remote(
            mixed_up.at[part, c], landed.at[part, chip],
            csend.at[part, c], crecv.at[part, chip], (2 * c + core, z),
        )

    def cross_arrive(part, c):
        return remote(
            mixed_up.at[part, c], landed.at[part, c],
            csend.at[part, c], crecv.at[part, c], (2 * c + core, z),
        )

    def g_send(peer):
        return remote(
            g_slice(g_ref, peer), g_land.at[z], gsend.at[peer], grecv.at[z], (me, peer)
        )

    def g_arrive(peer):
        return remote(
            g_slice(g_ref, peer), g_land.at[peer], gsend.at[peer], grecv.at[peer], (me, peer)
        )

    def h_send(peer):
        return remote(g_sum, g_slice(go_ref, z), hsend.at[peer], hrecv.at[z], (me, peer))

    def h_arrive(peer):
        return remote(g_sum, g_slice(go_ref, peer), hsend.at[peer], hrecv.at[peer], (me, peer))

    others = [lax.rem(chip + step, chips_n) for step in range(1, chips_n)]
    peers = [lax.rem(z + step, n_seq) for step in range(1, n_seq)]
    parts = p_ref.shape[0]
    for part in range(parts):
        for c in others + [chip]:
            pair_send(part, c).start()
    for peer in peers:
        g_send(peer).start()
    for part in range(parts):
        for c in others + [chip]:
            pair_send(part, c).wait_recv()
            mixed_up[part, c] = (
                p_ref[part, 2 * c + core].astype(F32) + pair[part, c].astype(F32)
            ).astype(BF16)
            if c is not chip:
                cross_send(part, c).start()
    total = g_slice(g_ref, z)[...].astype(F32)
    for peer in peers:
        g_arrive(peer).wait_recv()
        total = total + g_land[peer].astype(F32)
    g_sum[...] = total.astype(BF16)
    own_g = pltpu.make_async_copy(g_sum, g_slice(go_ref, z), local_sem.at[0])
    own_g.start()
    for peer in peers:
        h_send(peer).start()
    block, half = me % n_seq, me // n_seq
    src_core, sources = plane_sources(z)
    stream = 2 * ((1 - half) * sources[0] + half * sources[1]) + src_core
    stays = (stream == me) & (block == z)
    gone = jnp.logical_not(stays)
    home = plane_of(me)
    from_dp = (chip // 2) * n_seq + z
    arrives = jnp.logical_not((home == z) & (from_dp == me))

    def final_send(part):
        return remote(
            final.at[part], o_ref.at[part], osend.at[part], orecv.at[part], (stream, block)
        )

    def final_own(part):
        return pltpu.make_async_copy(final.at[part], o_ref.at[part], local_sem.at[1 + part])

    for part in range(parts):
        total = mixed_up[part, chip].astype(F32)
        for c in others:
            cross_arrive(part, c).wait_recv()
            total = total + landed[part, c].astype(F32)
        final[part] = total.astype(BF16)

        @pl.when(gone)
        def _():
            final_send(part).start()

        @pl.when(stays)
        def _():
            final_own(part).start()

    for part in range(parts):
        for c in others + [chip]:
            pair_send(part, c).wait_send()
        for c in others:
            cross_send(part, c).wait_send()

        @pl.when(gone)
        def _():
            final_send(part).wait_send()

        @pl.when(stays)
        def _():
            final_own(part).wait()

        @pl.when(arrives)
        def _():
            final_send(part).wait_recv()

    own_g.wait()
    for peer in peers:
        g_send(peer).wait_send()
        h_send(peer).wait_send()
        h_arrive(peer).wait_recv()


def mm(a, b, dims):
    return lax.dot_general(a, b, (dims, ((), ())), preferred_element_type=F32)


def forward_kernel(
    bias_ref, len_ref, proj_ref, srow_ref, scol_ref, att_ref, weight_ref, slope_ref
):
    length = len_ref[pl.program_id(0)]
    head = lax.axis_index("dp")
    total = proj_ref.shape[1]
    rows = total // 4
    acts = [jax.nn.silu(proj_ref[0, :, (1 + g) * DH : (2 + g) * DH]).astype(BF16) for g in range(3)]
    values, queries, keys = acts
    for start in range(0, total, rows):
        end = start + rows
        scores = mm(queries[start:end], keys[:end], ((1,), (1,))) * DH ** (-0.5)
        elapsed = scol_ref[0, start:end, :] - srow_ref[0, :, :end]
        bias = jnp.full(elapsed.shape, bias_ref[head, 0], F32)
        for degree in range(1, bias_ref.shape[1]):
            bias = jnp.where(elapsed >= 2**degree - 1, bias_ref[head, degree], bias)
        scores = scores + bias
        pos_q = start + lax.broadcasted_iota(jnp.int32, elapsed.shape, 0)
        pos_k = lax.broadcasted_iota(jnp.int32, elapsed.shape, 1)
        allowed = (pos_k <= pos_q) & (pos_k < length) & (pos_q < length)
        sig = jax.nn.sigmoid(scores)
        weight = jnp.where(allowed, scores * sig, 0.0).astype(BF16)
        weight_ref[0, start:end, :end] = weight
        slope_ref[0, start:end, :end] = jnp.where(allowed, sig * (1.0 + scores * (1.0 - sig)), 0.0)
        att_ref[0, start:end, :] = mm(weight, values[:end], ((1,), (0,)))


def backward_kernel(proj_ref, datt_ref, dgate_ref, weight_ref, slope_ref, out_ref, k_acc, v_acc):
    total = proj_ref.shape[1]
    rows = total // 4
    acts = [jax.nn.silu(proj_ref[0, :, (1 + g) * DH : (2 + g) * DH]).astype(BF16) for g in range(3)]
    values, queries, keys = acts
    scale = DH ** (-0.5)

    def put(group, start, end, grad):
        cols = slice(group * DH, (group + 1) * DH)
        out_ref[0, start:end, cols] = (grad * silu_slope(proj_ref[0, start:end, cols])).astype(BF16)

    for start in reversed(range(0, total, rows)):
        end = start + rows
        d_att = datt_ref[0, start:end, :]
        d_weight = mm(d_att, values[:end], ((1,), (1,)))
        d_scores = (d_weight * slope_ref[0, start:end, :end]).astype(BF16)
        put(2, start, end, mm(d_scores, keys[:end], ((1,), (0,))) * scale)
        k_part = mm(d_scores, queries[start:end], ((0,), (0,)))
        v_part = mm(weight_ref[0, start:end, :end], d_att, ((0,), (0,)))
        if end == total:
            k_acc[...] = k_part
            v_acc[...] = v_part
        else:
            k_acc[:end] += k_part
            v_acc[:end] += v_part
    put(0, 0, total, dgate_ref[0])
    put(1, 0, total, v_acc[...])
    put(3, 0, total, k_acc[...] * scale)


def head_parallel(
    n_dp, n_seq, tokens, cotangent, stamps, lengths, w_qkvu, w_out, gain_in, gain_out, bias_table
):
    tok, width = tokens.shape[1:]
    seq_len = stamps.shape[1]
    head = lax.axis_index("dp")
    meta = jnp.concatenate([stamps.reshape(-1, DH), jnp.broadcast_to(lengths[:, None], (4, DH))])
    w_cols = w_qkvu.reshape(-1, 4, n_dp, DH).transpose(2, 0, 1, 3).reshape(n_dp, -1, 4 * DH)
    dma = pltpu.SemaphoreType.DMA
    sds = jax.ShapeDtypeStruct
    side = pltpu.CompilerParams(has_side_effects=True)
    x_all, c_all, w_head, metas = pl.pallas_call(
        lambda *refs: gather_kernel(n_dp, n_seq, *refs),
        out_shape=(
            sds((2, n_seq, tok, width), BF16),
            sds((2, n_seq, tok, width), BF16),
            sds((n_dp, w_qkvu.shape[0], 4 * DH), BF16),
            sds((2,) + meta.shape, jnp.int32),
        ),
        in_specs=[VM] * 4,
        out_specs=[VM] * 4,
        scratch_shapes=[
            dma((2,)),
            dma((2, 2, n_seq, 3)),
            dma((2, 2, n_seq)),
            dma((n_dp,)),
            dma((n_dp,)),
            dma((n_dp,)),
            dma((2,)),
            dma((4,)),
        ],
        compiler_params=side,
        name="gather",
    )(tokens[0], cotangent[0], w_cols, meta)
    w_head = w_head.reshape(width, 4 * DH)
    count = 2 * seq_len
    x_rows = x_all.reshape(count, width)
    c_rows = c_all.reshape(count, width)
    stamp_rows = metas[:, : seq_len // DH].reshape(2, 1, seq_len)
    stamp_cols = stamp_rows.reshape(2, seq_len, 1)
    spans = metas[:, seq_len // DH, 0]
    normed = layer_norm(x_rows.astype(F32), gain_in).astype(BF16)
    projected = jnp.dot(normed, w_head, preferred_element_type=F32)
    proj3 = projected.reshape(2, seq_len, 4 * DH)
    smem = pl.BlockSpec(memory_space=pltpu.SMEM)

    def per(*shape):
        return pl.BlockSpec((1,) + shape, lambda i: (i,) + (0,) * len(shape))

    attended, weight, slope = pl.pallas_call(
        forward_kernel,
        grid=(2,),
        out_shape=(
            sds((2, seq_len, DH), F32),
            sds((2, seq_len, seq_len), BF16),
            sds((2, seq_len, seq_len), F32),
        ),
        in_specs=[smem, smem, per(seq_len, 4 * DH), per(1, seq_len), per(seq_len, 1)],
        out_specs=[per(seq_len, DH), per(seq_len, seq_len), per(seq_len, seq_len)],
        name="forward",
    )(bias_table, spans, proj3, stamp_rows, stamp_cols)
    att = attended.reshape(count, DH)
    gate = jax.nn.silu(projected[:, :DH])
    gain_head = lax.dynamic_slice_in_dim(gain_out, head * DH, DH)
    d_mix = lax.dot_general(c_rows, w_out, (((1,), (1,)), ((), ())), preferred_element_type=F32)
    g = d_mix * gate * gain_head
    mean_own = jnp.mean(att, axis=1)
    off = att - mean_own[:, None]
    stats = jnp.stack(
        [mean_own, jnp.sum(off * off, axis=1), jnp.sum(g, axis=1), jnp.sum(g * off, axis=1)]
    )
    gathered = pl.pallas_call(
        lambda *refs: stats_kernel(n_dp, *refs),
        out_shape=sds((n_dp, 4, count // DH, DH), F32),
        in_specs=[VM],
        out_specs=VM,
        scratch_shapes=[dma((n_dp,)), dma((n_dp,)), dma],
        compiler_params=side,
        name="stats",
    )(stats.reshape(4, count // DH, DH))
    means, squares, g_sums, g_offs = [gathered[:, k] for k in range(4)]
    mean = jnp.mean(means, axis=0)
    shift = means - mean[None]
    variance = jnp.sum(squares + DH * shift * shift, axis=0) / width
    rstd = lax.rsqrt(variance + EPS)
    g_mean = jnp.sum(g_sums, axis=0) / width
    g_dot = rstd * jnp.sum(g_offs + shift * g_sums, axis=0) / width
    mean, rstd, g_mean, g_dot = [v.reshape(count, 1) for v in (mean, rstd, g_mean, g_dot)]
    hat = (att - mean) * rstd
    normed_att = hat * gain_head
    mixed_rows = (normed_att * gate).astype(BF16)
    d_gate = d_mix * normed_att
    d_att = (rstd * (g - g_mean - hat * g_dot)).astype(BF16)
    d_proj = pl.pallas_call(
        backward_kernel,
        grid=(2,),
        out_shape=sds((2, seq_len, 4 * DH), BF16),
        in_specs=[
            per(seq_len, 4 * DH),
            per(seq_len, DH),
            per(seq_len, DH),
            per(seq_len, seq_len),
            per(seq_len, seq_len),
        ],
        out_specs=per(seq_len, 4 * DH),
        scratch_shapes=[pltpu.VMEM((seq_len, DH), F32)] * 2,
        name="backward",
    )(proj3, d_att.reshape(2, seq_len, DH), d_gate.reshape(2, seq_len, DH), weight, slope)
    mixed_part = jnp.dot(mixed_rows, w_out, preferred_element_type=F32).astype(BF16)
    d_part = lax.dot_general(
        d_proj.reshape(count, 4 * DH), w_head, (((1,), (1,)), ((), ())), preferred_element_type=F32
    ).astype(BF16)
    w_part = lax.dot_general(
        mixed_rows, c_rows, (((0,), (0,)), ((), ())), preferred_element_type=F32
    ).astype(BF16)
    shape = (n_dp, tok, width)
    half = n_dp // 2
    sums, w_sum = pl.pallas_call(
        lambda *refs: reduce_kernel(n_dp, n_seq, *refs),
        out_shape=(sds((2, tok, width), BF16), sds(w_part.shape, BF16)),
        in_specs=[VM] * 2,
        out_specs=[VM] * 2,
        scratch_shapes=[
            pltpu.VMEM((2, half, tok, width), BF16),
            pltpu.VMEM((2, half, tok, width), BF16),
            pltpu.VMEM((2, half, tok, width), BF16),
            pltpu.VMEM((2, tok, width), BF16),
            pltpu.VMEM((n_seq, w_part.shape[0] // n_seq, width), BF16),
            pltpu.VMEM((w_part.shape[0] // n_seq, width), BF16),
            dma((2, half)),
            dma((2, half)),
            dma((2, half)),
            dma((2, half)),
            dma((2,)),
            dma((2,)),
            dma((n_seq,)),
            dma((n_seq,)),
            dma((n_seq,)),
            dma((n_seq,)),
            dma((3,)),
        ],
        compiler_params=side,
        name="reduce",
    )(jnp.stack([mixed_part.reshape(shape), d_part.reshape(shape)]), w_part)
    wide_rows = tokens[0].astype(F32)
    mixed = (wide_rows + sums[0].astype(F32)).astype(BF16)
    unused_rows, in_back = jax.vjp(lambda values: layer_norm(values, gain_in), wide_rows)
    back = in_back(sums[1].astype(F32))[0]
    input_grad = (cotangent[0].astype(F32) + back).astype(BF16)
    return (mixed[None], input_grad[None], w_sum.astype(F32))


def solution(mesh):
    n_dp, n_seq = mesh.shape["dp"], mesh.shape["seq"]

    def body(*args):
        streams_fit = n_dp == 2 * n_seq and n_dp == H and args[5].shape[0] == DH
        if streams_fit and args[2].shape[0] == 1:
            return head_parallel(n_dp, n_seq, *args)
        return per_device(*args)

    return jax.shard_map(
        body,
        mesh=mesh,
        in_specs=(
            P("dp", "seq", None),
            P("dp", "seq", None),
            P("dp", None),
            P("dp"),
            P("dp", None),
            P("dp", None),
            P(),
            P(),
            P(),
        ),
        out_specs=(P("dp", "seq", None), P("dp", "seq", None), P("dp", None)),
        check_vma=False,
    )
```

```python
import jax
import jax.numpy as jnp
from jax import lax
from jax.experimental import pallas as pl
from jax.experimental.pallas import tpu as pltpu
from jax.sharding import PartitionSpec as P

H = 8
DH = 128


EPS = 1e-05


def layer_norm(values, gain):
    average = jnp.mean(values, axis=-1, keepdims=True)
    centred = values - average
    variance = jnp.mean(centred * centred, axis=-1, keepdims=True)
    return centred * lax.rsqrt(variance + EPS) * gain


def silu_slope(values):
    sigmoid_v = jax.nn.sigmoid(values)
    return sigmoid_v * (1.0 + values * (1.0 - sigmoid_v))


def time_bias(bias_table, stamps_q, stamps_k):
    elapsed = stamps_q[:, None] - stamps_k[None, :]
    bucket = jnp.zeros(elapsed.shape, jnp.int32)
    for degree in range(1, bias_table.shape[1]):
        bucket = bucket + (elapsed >= 2**degree - 1).astype(jnp.int32)
    levels = jnp.arange(bias_table.shape[1], dtype=jnp.int32)
    one_hot = (bucket[:, :, None] == levels[None, None, :]).astype(jnp.float32)
    return jnp.einsum(
        "qkb,hb->hqk",
        one_hot,
        bias_table,
        precision=lax.Precision.HIGHEST,
        preferred_element_type=jnp.float32,
    )


def pair_terms(
    q_heads, d_heads, stamps_q, pos_q, k_heads, v_heads, stamps_k, pos_k, length, bias_table, scale
):
    scores = (
        jnp.einsum("qhd,khd->hqk", q_heads, k_heads, preferred_element_type=jnp.float32) * scale
    )
    scores = scores + time_bias(bias_table, stamps_q, stamps_k)
    allowed = (
        (pos_k[None, :] <= pos_q[:, None]) & (pos_k[None, :] < length) & (pos_q[:, None] < length)
    )
    weight = jnp.where(allowed[None], jax.nn.silu(scores), 0.0).astype(jnp.bfloat16)
    if d_heads is None:
        return (weight, None)
    d_weight = jnp.einsum("qhd,khd->hqk", d_heads, v_heads, preferred_element_type=jnp.float32)
    d_scores = jnp.where(allowed[None], d_weight * silu_slope(scores), 0.0).astype(jnp.bfloat16)
    return (weight, d_scores)


def per_device(tokens, cotangent, stamps, lengths, w_qkvu, w_out, gain_in, gain_out, bias_table):
    rows = tokens[0]
    cot_rows = cotangent[0]
    tok_count = rows.shape[0]
    feature_width = rows.shape[1]
    seq_count = lax.axis_size("seq")
    total_rows = tok_count * seq_count
    first_row = lax.axis_index("seq") * tok_count
    length = lengths[0]
    stamp_all = stamps[0]
    pos_own = first_row + jnp.arange(tok_count, dtype=jnp.int32)
    stamp_own = lax.dynamic_slice_in_dim(stamp_all, first_row, tok_count)
    scale = DH ** (-0.5)
    block_rows = min(512, total_rows)
    block_count = total_rows // block_rows
    w_full, w_out_full = (
        lax.all_gather(w_qkvu, "dp", axis=0, tiled=True),
        lax.all_gather(w_out, "dp", axis=0, tiled=True),
    )
    wide_rows = rows.astype(jnp.float32)
    normed = layer_norm(wide_rows, gain_in).astype(jnp.bfloat16)
    projected = jnp.dot(normed, w_full, preferred_element_type=jnp.float32)
    activated = jax.nn.silu(projected)
    gate_u = activated[:, :feature_width]
    values_own = activated[:, feature_width : 2 * feature_width].astype(jnp.bfloat16)
    queries_own = activated[:, 2 * feature_width : 3 * feature_width].astype(jnp.bfloat16)
    keys_own = activated[:, 3 * feature_width :].astype(jnp.bfloat16)
    keys_all, values_all = (
        lax.all_gather(keys_own, "seq", axis=0, tiled=True),
        lax.all_gather(values_own, "seq", axis=0, tiled=True),
    )
    q_heads = queries_own.reshape(tok_count, H, DH)

    def key_block(start):
        k_heads = lax.dynamic_slice_in_dim(keys_all, start, block_rows).reshape(block_rows, H, DH)
        v_heads = lax.dynamic_slice_in_dim(values_all, start, block_rows).reshape(block_rows, H, DH)
        stamps_k = lax.dynamic_slice_in_dim(stamp_all, start, block_rows)
        pos_k = start + jnp.arange(block_rows, dtype=jnp.int32)
        return (k_heads, v_heads, stamps_k, pos_k)

    def guarded(active, action, state):
        return lax.cond(active, action, lambda same: same, state)

    def reaches(start):
        return (start <= first_row + tok_count - 1) & (start < length) & (first_row < length)

    def forward_step(block_idx, totals):
        start = block_idx * block_rows

        def forward_compute(totals):
            k_heads, v_heads, stamps_k, pos_k = key_block(start)
            weight, unused = pair_terms(
                q_heads,
                None,
                stamp_own,
                pos_own,
                k_heads,
                v_heads,
                stamps_k,
                pos_k,
                length,
                bias_table,
                scale,
            )
            return totals + jnp.einsum(
                "hqk,khd->qhd", weight, v_heads, preferred_element_type=jnp.float32
            )

        return guarded(reaches(start), forward_compute, totals)

    attended = lax.fori_loop(
        0, block_count, forward_step, jnp.zeros((tok_count, H, DH), jnp.float32)
    )
    attended = attended.reshape(tok_count, feature_width)
    normed_att, norm_back = jax.vjp(lambda values: layer_norm(values, gain_out), attended)
    mixed_rows = (normed_att * gate_u).astype(jnp.bfloat16)
    mixed = (
        wide_rows + jnp.dot(mixed_rows, w_out_full, preferred_element_type=jnp.float32)
    ).astype(jnp.bfloat16)
    grad_part = lax.psum_scatter(
        jnp.einsum("tr,tc->rc", mixed_rows, cot_rows, preferred_element_type=jnp.float32).astype(
            jnp.bfloat16
        ),
        "dp",
        scatter_dimension=0,
        tiled=True,
    )
    w_grad = lax.psum(grad_part, "seq").astype(jnp.float32)
    d_mix = jnp.einsum("tc,rc->tr", cot_rows, w_out_full, preferred_element_type=jnp.float32)
    d_gate = d_mix * normed_att
    d_att = norm_back(d_mix * gate_u)[0].astype(jnp.bfloat16)
    d_heads = d_att.reshape(tok_count, H, DH)

    def backward_step():

        def step(block_idx, state_pair):
            start = block_idx * block_rows

            def step_compute(state_pair):
                q_grad, key_terms = state_pair
                k_heads, v_heads, stamps_k, pos_k = key_block(start)
                weight, d_scores = pair_terms(
                    q_heads,
                    d_heads,
                    stamp_own,
                    pos_own,
                    k_heads,
                    v_heads,
                    stamps_k,
                    pos_k,
                    length,
                    bias_table,
                    scale,
                )
                q_grad = (
                    q_grad
                    + jnp.einsum(
                        "hqk,khd->qhd", d_scores, k_heads, preferred_element_type=jnp.float32
                    )
                    * scale
                )
                k_grad = (
                    jnp.einsum(
                        "hqk,qhd->khd", d_scores, q_heads, preferred_element_type=jnp.float32
                    )
                    * scale
                )
                v_grad = jnp.einsum(
                    "hqk,qhd->khd", weight, d_heads, preferred_element_type=jnp.float32
                )
                joined = jnp.concatenate(
                    [
                        k_grad.reshape(block_rows, feature_width),
                        v_grad.reshape(block_rows, feature_width),
                    ],
                    axis=1,
                )
                key_terms = lax.dynamic_update_slice_in_dim(key_terms, joined, start, 0)
                return (q_grad, key_terms)

            return guarded(reaches(start), step_compute, state_pair)

        return step

    q_start = jnp.zeros((tok_count, H, DH), jnp.float32)
    term_start = jnp.zeros((total_rows, 2 * feature_width), jnp.float32)
    q_grad, key_terms = lax.fori_loop(0, block_count, backward_step(), (q_start, term_start))
    key_grads = lax.psum_scatter(
        key_terms.astype(jnp.bfloat16), "seq", scatter_dimension=0, tiled=True
    ).astype(jnp.float32)
    d_act = jnp.concatenate(
        [
            d_gate,
            key_grads[:, feature_width:],
            q_grad.reshape(tok_count, feature_width),
            key_grads[:, :feature_width],
        ],
        axis=1,
    )
    d_proj = (d_act * silu_slope(projected)).astype(jnp.bfloat16)
    d_normed = jnp.einsum("tf,df->td", d_proj, w_full, preferred_element_type=jnp.float32)
    unused_rows, in_back = jax.vjp(lambda values: layer_norm(values, gain_in), wide_rows)
    input_grad = (cot_rows.astype(jnp.float32) + in_back(d_normed)[0]).astype(jnp.bfloat16)
    return (mixed[None], input_grad[None], w_grad)


MESH = pl.DeviceIdType.MESH
VM = pl.BlockSpec(memory_space=pltpu.VMEM)
F32 = jnp.float32
BF16 = jnp.bfloat16


def plane_of(stream):
    chip, core = stream // 2, stream % 2
    mid = 1 - ((chip + 1) // 2) % 2
    return mid * (1 + core) + (1 - mid) * 3 * core


def plane_sources(plane):
    mid = ((plane + 1) // 2) % 2
    core = mid * (plane - 1) + (1 - mid) * (plane // 3)
    return core, (1 - mid, 2 + mid)


def remote(src, dst, send_sem, recv_sem, target):
    return pltpu.make_async_remote_copy(
        src_ref=src,
        dst_ref=dst,
        send_sem=send_sem,
        recv_sem=recv_sem,
        device_id=target,
        device_id_type=MESH,
    )


def gather_kernel(
    n_dp, n_seq, x_ref, c_ref, w_ref, m_ref, gain_ref, proj_ref, co_ref, wo_ref, mo_ref, xo_ref,
    zsend, fsend, frecv, wsend, wrecv, msend, mrecv, local_sem,
):
    me = lax.axis_index("dp")
    z = lax.axis_index("seq")
    chip, core = me // 2, me % 2
    cy, cx = chip // 2, chip % 2
    x_chip, y_chip = 2 * cy + (1 - cx), 2 * (1 - cy) + cx
    sibling = 2 * chip + (1 - core)
    home = plane_of(me)
    slot = chip // 2
    src_core, chips = plane_sources(z)
    ins, outs = (x_ref, c_ref), (xo_ref, co_ref)

    def z_send(a, s):
        return remote(ins[a], outs[a].at[slot, s], zsend.at[a], frecv.at[a, slot, s], (me, home))

    def own_copy(a):
        return pltpu.make_async_copy(ins[a], outs[a].at[slot, z], local_sem.at[a])

    def w_send(peer):
        return remote(w_ref.at[peer], wo_ref.at[me], wsend.at[peer], wrecv.at[me], (peer, z))

    def w_arrive(peer):
        return remote(w_ref.at[peer], wo_ref.at[peer], wsend.at[peer], wrecv.at[peer], (peer, z))

    def w_own():
        return pltpu.make_async_copy(w_ref.at[me], wo_ref.at[me], local_sem.at[3])

    def m_send(peer):
        return remote(m_ref, mo_ref.at[slot], msend.at[peer], mrecv.at[slot], (peer, z))

    def m_own():
        return pltpu.make_async_copy(m_ref, mo_ref.at[slot], local_sem.at[2])

    @pl.when(home != z)
    def _():
        z_send(0, z).start()

    @pl.when(home == z)
    def _():
        own_copy(0).start()
        m_own().start()

    for step in range(1, n_dp):
        peer = lax.rem(me + step, n_dp)

        @pl.when(home == z)
        def _():
            m_send(peer).start()

        w_send(peer).start()
    w_own().start()

    @pl.when(home != z)
    def _():
        z_send(1, z).start()

    @pl.when(home == z)
    def _():
        own_copy(1).start()

    def order(i):
        return lax.rem(z + i, n_seq)

    def pass_on(a, j, b, target, leg):
        block = outs[a].at[j, b]
        return remote(block, block, fsend.at[a, j, b, leg], frecv.at[a, j, b], (target, z))

    def from_source(a, i):
        b = order(i)
        return (
            pass_on(a, slot, b, 2 * x_chip + core, 0),
            pass_on(a, slot, b, 2 * y_chip + core, 1),
            pass_on(a, slot, b, sibling, 2),
        )

    is_source = home == z
    relays = core == src_core

    def relayed(a, i, j):
        b = order(i)
        if i % 2 == 0:
            return relays & (x_chip == chips[j]), pass_on(a, j, b, 2 * y_chip + core, 1)
        return relays & (y_chip == chips[j]), pass_on(a, j, b, 2 * x_chip + core, 0)

    def shared(a, i, j):
        return relays & (chip != chips[j]), pass_on(a, j, order(i), sibling, 2)

    for a in range(2):

        @pl.when(is_source)
        def _():
            for i in range(n_seq):
                if i == 0:
                    own_copy(a).wait()
                else:
                    pass_on(a, slot, order(i), me, 0).wait_recv()
                for copy in from_source(a, i):
                    copy.start()

    def project(i, j):
        b = order(i)
        normed = layer_norm(xo_ref[j, b].astype(F32), gain_ref[...]).astype(BF16)
        weights = wo_ref[...].reshape(-1, 4 * DH)
        proj_ref[j, b] = jnp.dot(normed, weights, preferred_element_type=F32)

    for a in range(2):
        for i in range(n_seq):
            for j in range(2):

                @pl.when(jnp.logical_not(is_source & (slot == j)))
                def _():
                    pass_on(a, j, order(i), me, 0).wait_recv()

                for use, copy in (relayed(a, i, j), shared(a, i, j)):

                    @pl.when(use)
                    def _():
                        copy.start()

                if a == 1:
                    project(i, j)

        if a == 0:
            w_own().wait()
            for step in range(1, n_dp):
                w_arrive(lax.rem(me + step, n_dp)).wait_recv()

    for step in range(1, n_dp):
        peer = lax.rem(me + step, n_dp)
        w_send(peer).wait_send()

        @pl.when(home == z)
        def _():
            m_send(peer).wait_send()

    @pl.when(home == z)
    def _():
        m_own().wait()

    for j in range(2):

        @pl.when(jnp.logical_not((home == z) & (slot == j)))
        def _():
            remote(m_ref, mo_ref.at[j], msend.at[0], mrecv.at[j], (me, z)).wait_recv()

    for a in range(2):

        @pl.when(home != z)
        def _():
            z_send(a, z).wait_send()

        @pl.when(is_source)
        def _():
            for i in range(n_seq):
                for copy in from_source(a, i):
                    copy.wait_send()

        for i in range(n_seq):
            for j in range(2):
                for use, copy in (relayed(a, i, j), shared(a, i, j)):

                    @pl.when(use)
                    def _():
                        copy.wait_send()


def stats_kernel(n_dp, s_ref, o_ref, send, recv, local_sem):
    me = lax.axis_index("dp")
    z = lax.axis_index("seq")
    barrier = pltpu.get_barrier_semaphore()
    for step in range(1, n_dp):
        pl.semaphore_signal(
            barrier, inc=1, device_id=(lax.rem(me + step, n_dp), z), device_id_type=MESH
        )
    pl.semaphore_wait(barrier, n_dp - 1)
    own = pltpu.make_async_copy(s_ref, o_ref.at[me], local_sem)
    own.start()
    for step in range(1, n_dp):
        peer = lax.rem(me + step, n_dp)
        remote(s_ref, o_ref.at[me], send.at[peer], recv.at[me], (peer, z)).start()
    own.wait()
    for step in range(1, n_dp):
        peer = lax.rem(me + step, n_dp)
        copy = remote(s_ref, o_ref.at[peer], send.at[peer], recv.at[peer], (peer, z))
        copy.wait_recv()
        copy.wait_send()


def reduce_kernel(
    n_dp, n_seq, pm_ref, pd_ref, g_ref, o_ref, go_ref, pair, mixed_up, landed, final, g_land, g_sum,
    psend, precv, csend, crecv, osend, orecv, gsend, grecv, hsend, hrecv, local_sem,
):
    me = lax.axis_index("dp")
    z = lax.axis_index("seq")
    chip, core = me // 2, me % 2
    sibling = 2 * chip + (1 - core)
    chips_n = n_dp // 2
    g_rows = g_ref.shape[0] // n_seq
    p_refs = (pm_ref, pd_ref)

    def g_slice(ref, index):
        return ref.at[pl.ds(pl.multiple_of(index * g_rows, g_rows), g_rows)]

    def pair_send(part, c):
        return remote(
            p_refs[part].at[2 * c + (1 - core)], pair.at[part, c],
            psend.at[part, c], precv.at[part, c], (sibling, z),
        )

    def cross_send(part, c):
        return remote(
            mixed_up.at[part, c], landed.at[part, chip],
            csend.at[part, c], crecv.at[part, chip], (2 * c + core, z),
        )

    def cross_arrive(part, c):
        return remote(
            mixed_up.at[part, c], landed.at[part, c],
            csend.at[part, c], crecv.at[part, c], (2 * c + core, z),
        )

    def g_send(peer):
        return remote(
            g_slice(g_ref, peer), g_land.at[z], gsend.at[peer], grecv.at[z], (me, peer)
        )

    def g_arrive(peer):
        return remote(
            g_slice(g_ref, peer), g_land.at[peer], gsend.at[peer], grecv.at[peer], (me, peer)
        )

    def h_send(peer):
        return remote(g_sum, g_slice(go_ref, z), hsend.at[peer], hrecv.at[z], (me, peer))

    def h_arrive(peer):
        return remote(g_sum, g_slice(go_ref, peer), hsend.at[peer], hrecv.at[peer], (me, peer))

    others = [lax.rem(chip + step, chips_n) for step in range(1, chips_n)]
    peers = [lax.rem(z + step, n_seq) for step in range(1, n_seq)]
    parts = len(p_refs)
    for part in range(parts):
        for c in others + [chip]:
            pair_send(part, c).start()
    for peer in peers:
        g_send(peer).start()
    for part in range(parts):
        for c in others + [chip]:
            pair_send(part, c).wait_recv()
            mixed_up[part, c] = (
                p_refs[part][2 * c + core].astype(F32) + pair[part, c].astype(F32)
            ).astype(BF16)
            if c is not chip:
                cross_send(part, c).start()
    total = g_slice(g_ref, z)[...].astype(F32)
    for peer in peers:
        g_arrive(peer).wait_recv()
        total = total + g_land[peer].astype(F32)
    g_sum[...] = total.astype(BF16)
    own_g = pltpu.make_async_copy(g_sum, g_slice(go_ref, z), local_sem.at[0])
    own_g.start()
    for peer in peers:
        h_send(peer).start()
    block, half = me % n_seq, me // n_seq
    src_core, sources = plane_sources(z)
    stream = 2 * ((1 - half) * sources[0] + half * sources[1]) + src_core
    stays = (stream == me) & (block == z)
    gone = jnp.logical_not(stays)
    home = plane_of(me)
    from_dp = (chip // 2) * n_seq + z
    arrives = jnp.logical_not((home == z) & (from_dp == me))

    def final_send(part):
        return remote(
            final.at[part], o_ref.at[part], osend.at[part], orecv.at[part], (stream, block)
        )

    def final_own(part):
        return pltpu.make_async_copy(final.at[part], o_ref.at[part], local_sem.at[1 + part])

    for part in range(parts):
        total = mixed_up[part, chip].astype(F32)
        for c in others:
            cross_arrive(part, c).wait_recv()
            total = total + landed[part, c].astype(F32)
        final[part] = total.astype(BF16)

        @pl.when(gone)
        def _():
            final_send(part).start()

        @pl.when(stays)
        def _():
            final_own(part).start()

    for part in range(parts):
        for c in others + [chip]:
            pair_send(part, c).wait_send()
        for c in others:
            cross_send(part, c).wait_send()

        @pl.when(gone)
        def _():
            final_send(part).wait_send()

        @pl.when(stays)
        def _():
            final_own(part).wait()

        @pl.when(arrives)
        def _():
            final_send(part).wait_recv()

    own_g.wait()
    for peer in peers:
        g_send(peer).wait_send()
        h_send(peer).wait_send()
        h_arrive(peer).wait_recv()


def mm(a, b, dims):
    return lax.dot_general(a, b, (dims, ((), ())), preferred_element_type=F32)


def forward_kernel(
    bias_ref, len_ref, proj_ref, srow_ref, scol_ref, att_ref, weight_ref, slope_ref
):
    length = len_ref[pl.program_id(0)]
    head = lax.axis_index("dp")
    total = proj_ref.shape[1]
    rows = total // 4
    acts = [jax.nn.silu(proj_ref[0, :, (1 + g) * DH : (2 + g) * DH]).astype(BF16) for g in range(3)]
    values, queries, keys = acts
    for start in range(0, total, rows):
        end = start + rows
        scores = mm(queries[start:end], keys[:end], ((1,), (1,))) * DH ** (-0.5)
        elapsed = scol_ref[0, start:end, :] - srow_ref[0, :, :end]
        bias = jnp.full(elapsed.shape, bias_ref[head, 0], F32)
        for degree in range(1, bias_ref.shape[1]):
            bias = jnp.where(elapsed >= 2**degree - 1, bias_ref[head, degree], bias)
        scores = scores + bias
        pos_q = start + lax.broadcasted_iota(jnp.int32, elapsed.shape, 0)
        pos_k = lax.broadcasted_iota(jnp.int32, elapsed.shape, 1)
        allowed = (pos_k <= pos_q) & (pos_k < length) & (pos_q < length)
        sig = jax.nn.sigmoid(scores)
        weight = jnp.where(allowed, scores * sig, 0.0).astype(BF16)
        weight_ref[0, start:end, :end] = weight
        slope_ref[0, start:end, :end] = jnp.where(allowed, sig * (1.0 + scores * (1.0 - sig)), 0.0)
        att_ref[0, start:end, :] = mm(weight, values[:end], ((1,), (0,)))


def backward_kernel(proj_ref, datt_ref, dgate_ref, weight_ref, slope_ref, out_ref, k_acc, v_acc):
    total = proj_ref.shape[1]
    rows = total // 4
    acts = [jax.nn.silu(proj_ref[0, :, (1 + g) * DH : (2 + g) * DH]).astype(BF16) for g in range(3)]
    values, queries, keys = acts
    scale = DH ** (-0.5)

    def put(group, start, end, grad):
        cols = slice(group * DH, (group + 1) * DH)
        out_ref[0, start:end, cols] = (grad * silu_slope(proj_ref[0, start:end, cols])).astype(BF16)

    for start in reversed(range(0, total, rows)):
        end = start + rows
        d_att = datt_ref[0, start:end, :]
        d_weight = mm(d_att, values[:end], ((1,), (1,)))
        d_scores = (d_weight * slope_ref[0, start:end, :end]).astype(BF16)
        put(2, start, end, mm(d_scores, keys[:end], ((1,), (0,))) * scale)
        k_part = mm(d_scores, queries[start:end], ((0,), (0,)))
        v_part = mm(weight_ref[0, start:end, :end], d_att, ((0,), (0,)))
        if end == total:
            k_acc[...] = k_part
            v_acc[...] = v_part
        else:
            k_acc[:end] += k_part
            v_acc[:end] += v_part
    put(0, 0, total, dgate_ref[0])
    put(1, 0, total, v_acc[...])
    put(3, 0, total, k_acc[...] * scale)


def head_parallel(
    n_dp, n_seq, tokens, cotangent, stamps, lengths, w_qkvu, w_out, gain_in, gain_out, bias_table
):
    tok, width = tokens.shape[1:]
    seq_len = stamps.shape[1]
    head = lax.axis_index("dp")
    meta = jnp.concatenate([stamps.reshape(-1, DH), jnp.broadcast_to(lengths[:, None], (4, DH))])
    w_cols = w_qkvu.reshape(-1, 4, n_dp, DH).transpose(2, 0, 1, 3).reshape(n_dp, -1, 4 * DH)
    dma = pltpu.SemaphoreType.DMA
    sds = jax.ShapeDtypeStruct
    side = pltpu.CompilerParams(has_side_effects=True)
    projected, c_all, w_head, metas = pl.pallas_call(
        lambda *refs: gather_kernel(n_dp, n_seq, *refs),
        out_shape=(
            sds((2, n_seq, tok, 4 * DH), F32),
            sds((2, n_seq, tok, width), BF16),
            sds((n_dp, w_qkvu.shape[0], 4 * DH), BF16),
            sds((2,) + meta.shape, jnp.int32),
        ),
        in_specs=[VM] * 5,
        out_specs=[VM] * 4,
        scratch_shapes=[
            pltpu.VMEM((2, n_seq, tok, width), BF16),
            dma((2,)),
            dma((2, 2, n_seq, 3)),
            dma((2, 2, n_seq)),
            dma((n_dp,)),
            dma((n_dp,)),
            dma((n_dp,)),
            dma((2,)),
            dma((4,)),
        ],
        compiler_params=side,
        name="gather",
    )(tokens[0], cotangent[0], w_cols, meta, gain_in[None])
    w_head = w_head.reshape(width, 4 * DH)
    count = 2 * seq_len
    c_rows = c_all.reshape(count, width)
    stamp_rows = metas[:, : seq_len // DH].reshape(2, 1, seq_len)
    stamp_cols = stamp_rows.reshape(2, seq_len, 1)
    spans = metas[:, seq_len // DH, 0]
    projected = projected.reshape(count, 4 * DH)
    proj3 = projected.reshape(2, seq_len, 4 * DH)
    smem = pl.BlockSpec(memory_space=pltpu.SMEM)

    def per(*shape):
        return pl.BlockSpec((1,) + shape, lambda i: (i,) + (0,) * len(shape))

    attended, weight, slope = pl.pallas_call(
        forward_kernel,
        grid=(2,),
        out_shape=(
            sds((2, seq_len, DH), F32),
            sds((2, seq_len, seq_len), BF16),
            sds((2, seq_len, seq_len), F32),
        ),
        in_specs=[smem, smem, per(seq_len, 4 * DH), per(1, seq_len), per(seq_len, 1)],
        out_specs=[per(seq_len, DH), per(seq_len, seq_len), per(seq_len, seq_len)],
        name="forward",
    )(bias_table, spans, proj3, stamp_rows, stamp_cols)
    att = attended.reshape(count, DH)
    gate = jax.nn.silu(projected[:, :DH])
    gain_head = lax.dynamic_slice_in_dim(gain_out, head * DH, DH)
    d_mix = lax.dot_general(c_rows, w_out, (((1,), (1,)), ((), ())), preferred_element_type=F32)
    g = d_mix * gate * gain_head
    mean_own = jnp.mean(att, axis=1)
    off = att - mean_own[:, None]
    stats = jnp.stack(
        [mean_own, jnp.sum(off * off, axis=1), jnp.sum(g, axis=1), jnp.sum(g * off, axis=1)]
    )
    gathered = pl.pallas_call(
        lambda *refs: stats_kernel(n_dp, *refs),
        out_shape=sds((n_dp, 4, count // DH, DH), F32),
        in_specs=[VM],
        out_specs=VM,
        scratch_shapes=[dma((n_dp,)), dma((n_dp,)), dma],
        compiler_params=pltpu.CompilerParams(has_side_effects=True, collective_id=1),
        name="stats",
    )(stats.reshape(4, count // DH, DH))
    means, squares, g_sums, g_offs = [gathered[:, k] for k in range(4)]
    mean = jnp.mean(means, axis=0)
    shift = means - mean[None]
    variance = jnp.sum(squares + DH * shift * shift, axis=0) / width
    rstd = lax.rsqrt(variance + EPS)
    g_mean = jnp.sum(g_sums, axis=0) / width
    g_dot = rstd * jnp.sum(g_offs + shift * g_sums, axis=0) / width
    mean, rstd, g_mean, g_dot = [v.reshape(count, 1) for v in (mean, rstd, g_mean, g_dot)]
    hat = (att - mean) * rstd
    normed_att = hat * gain_head
    mixed_rows = (normed_att * gate).astype(BF16)
    d_gate = d_mix * normed_att
    d_att = (rstd * (g - g_mean - hat * g_dot)).astype(BF16)
    d_proj = pl.pallas_call(
        backward_kernel,
        grid=(2,),
        out_shape=sds((2, seq_len, 4 * DH), BF16),
        in_specs=[
            per(seq_len, 4 * DH),
            per(seq_len, DH),
            per(seq_len, DH),
            per(seq_len, seq_len),
            per(seq_len, seq_len),
        ],
        out_specs=per(seq_len, 4 * DH),
        scratch_shapes=[pltpu.VMEM((seq_len, DH), F32)] * 2,
        name="backward",
    )(proj3, d_att.reshape(2, seq_len, DH), d_gate.reshape(2, seq_len, DH), weight, slope)
    mixed_part = jnp.dot(mixed_rows, w_out, preferred_element_type=F32).astype(BF16)
    d_part = lax.dot_general(
        d_proj.reshape(count, 4 * DH), w_head, (((1,), (1,)), ((), ())), preferred_element_type=F32
    ).astype(BF16)
    w_part = lax.dot_general(
        mixed_rows, c_rows, (((0,), (0,)), ((), ())), preferred_element_type=F32
    ).astype(BF16)
    shape = (n_dp, tok, width)
    half = n_dp // 2
    sums, w_sum = pl.pallas_call(
        lambda *refs: reduce_kernel(n_dp, n_seq, *refs),
        out_shape=(sds((2, tok, width), BF16), sds(w_part.shape, BF16)),
        in_specs=[VM] * 3,
        out_specs=[VM] * 2,
        scratch_shapes=[
            pltpu.VMEM((2, half, tok, width), BF16),
            pltpu.VMEM((2, half, tok, width), BF16),
            pltpu.VMEM((2, half, tok, width), BF16),
            pltpu.VMEM((2, tok, width), BF16),
            pltpu.VMEM((n_seq, w_part.shape[0] // n_seq, width), BF16),
            pltpu.VMEM((w_part.shape[0] // n_seq, width), BF16),
            dma((2, half)),
            dma((2, half)),
            dma((2, half)),
            dma((2, half)),
            dma((2,)),
            dma((2,)),
            dma((n_seq,)),
            dma((n_seq,)),
            dma((n_seq,)),
            dma((n_seq,)),
            dma((3,)),
        ],
        compiler_params=side,
        name="reduce",
    )(mixed_part.reshape(shape), d_part.reshape(shape), w_part)
    wide_rows = tokens[0].astype(F32)
    mixed = (wide_rows + sums[0].astype(F32)).astype(BF16)
    unused_rows, in_back = jax.vjp(lambda values: layer_norm(values, gain_in), wide_rows)
    back = in_back(sums[1].astype(F32))[0]
    input_grad = (cotangent[0].astype(F32) + back).astype(BF16)
    return (mixed[None], input_grad[None], w_sum.astype(F32))


def solution(mesh):
    n_dp, n_seq = mesh.shape["dp"], mesh.shape["seq"]

    def body(*args):
        streams_fit = n_dp == 2 * n_seq and n_dp == H and args[5].shape[0] == DH
        if streams_fit and args[2].shape[0] == 1:
            return head_parallel(n_dp, n_seq, *args)
        return per_device(*args)

    return jax.shard_map(
        body,
        mesh=mesh,
        in_specs=(
            P("dp", "seq", None),
            P("dp", "seq", None),
            P("dp", None),
            P("dp"),
            P("dp", None),
            P("dp", None),
            P(),
            P(),
            P(),
        ),
        out_specs=(P("dp", "seq", None), P("dp", "seq", None), P("dp", None)),
        check_vma=False,
    )
```
